32 devices in a mesh: cp: 32 (over z, y, x, core).
Axes of the slice: x: 2, y: 2, z: 4, core: 2. Of those that a mesh axis runs over, the one named last changes fastest.
Arguments:
- u_in: bfloat16 [16, 2048, 5376], P(None, 'cp')
- seg_ids: int32 [16, 2048], P(None, 'cp')
- grad_h: float32 [16, 2048, 5376], P(None, 'cp')
- conv_w: float32 [4, 5376], replicated
- conv_b: float32 [5376], replicated
- a_gate_w: bfloat16 [21, 256, 256], replicated
- a_gate_b: float32 [5376], replicated
- x_gate_w: bfloat16 [21, 256, 256], replicated
- x_gate_b: float32 [5376], replicated
- lam_param: float32 [5376], replicated
Outputs:
- output 1: bfloat16 [16, 2048, 5376], P(None, 'cp')
- output 2: float32 [4, 5376], replicated
- output 3: float32 [5376], replicated
- output 4: float32 [21, 256, 256], replicated
- output 5: float32 [5376], replicated
- output 6: float32 [21, 256, 256], replicated
- output 7: float32 [5376], replicated
- output 8: float32 [5376], replicated
All inputs are finite; a program needn't handle non-finite values.
Results may differ from the reference program's by a relative error of at most 0.001.
Values sent between devices are 32-bit elements.
A program may use at most 1 GiB of HBM per device.

```python
import jax
import jax.numpy as jnp
from jax import lax

BATCH = 16
TOK_DEV = 64
CP_SIZE = 32
D_RNN = 5376
HEADS = 21
CONV = 4
SEQ = CP_SIZE * TOK_DEV
BLOCK_W = D_RNN // HEADS


def setup_inputs(seed: int = 0) -> dict:
    root_key = jax.random.key(seed)
    key_list = jax.random.split(root_key, 10)
    u_in = jax.random.normal(key_list[0], (BATCH, SEQ, D_RNN), jnp.float32).astype(jnp.bfloat16)
    starts = jax.random.randint(key_list[1], (BATCH, SEQ), 0, 2 * TOK_DEV) == 0
    starts = starts | (jnp.arange(SEQ) == 0)[None, :]
    seg_ids = jnp.cumsum(starts.astype(jnp.int32), axis=1).astype(jnp.int32)
    grad_h = jax.random.normal(key_list[2], (BATCH, SEQ, D_RNN), jnp.float32)
    conv_w = 0.5 * jax.random.normal(key_list[3], (CONV, D_RNN), jnp.float32)
    conv_b = 0.5 * jax.random.normal(key_list[4], (D_RNN,), jnp.float32)
    w_scale = BLOCK_W ** -0.5
    a_gate_w = (w_scale * jax.random.normal(key_list[5], (HEADS, BLOCK_W, BLOCK_W), jnp.float32)).astype(jnp.bfloat16)
    a_gate_b = jax.random.normal(key_list[6], (D_RNN,), jnp.float32)
    x_gate_w = (w_scale * jax.random.normal(key_list[7], (HEADS, BLOCK_W, BLOCK_W), jnp.float32)).astype(jnp.bfloat16)
    x_gate_b = jax.random.normal(key_list[8], (D_RNN,), jnp.float32)
    kappa_val = jax.random.uniform(key_list[9], (D_RNN,), jnp.float32, 0.3, 3.0)
    lam_param = -jnp.log(jnp.expm1(kappa_val / (8.0 * TOK_DEV)))
    return {'u_in': u_in, 'seg_ids': seg_ids, 'grad_h': grad_h, 'conv_w': conv_w, 'conv_b': conv_b,
            'a_gate_w': a_gate_w, 'a_gate_b': a_gate_b, 'x_gate_w': x_gate_w, 'x_gate_b': x_gate_b,
            'lam_param': lam_param}


def lru_scan(conv_out, pre_a, pre_i, lam_param, reset):
    gate_r = jax.nn.sigmoid(pre_a)
    gate_i = jax.nn.sigmoid(pre_i)
    log_a = -8.0 * gate_r * jax.nn.softplus(-lam_param)
    decay_a = jnp.where(reset, 0.0, jnp.exp(log_a))
    multiplier = jnp.where(reset, 1.0, jnp.sqrt(-jnp.expm1(2.0 * log_a)))
    x_t = multiplier * gate_i * conv_out

    def step_fn(run_state, step_in):
        dec_t, inp_t = step_in
        run_state = dec_t * run_state + inp_t
        return run_state, run_state

    _, hidden = lax.scan(step_fn, jnp.zeros_like(conv_out[0]), (decay_a, x_t))
    return hidden


def row_grads(u_row, seg_row, grad_row, conv_w, conv_b, a_gate_w, a_gate_b, x_gate_w, x_gate_b, lam_param):
    positions = jnp.arange(SEQ)
    mask_list = []
    conv_out = jnp.zeros((SEQ, D_RNN), jnp.float32) + conv_b
    for offset in range(CONV):
        u_shift = jnp.pad(u_row, ((offset, 0), (0, 0)))[:SEQ].astype(jnp.float32)
        seg_shift = jnp.pad(seg_row, (offset, 0), constant_values=-1)[:SEQ]
        tap_ok = ((seg_shift == seg_row) & (positions >= offset))[:, None]
        mask_list.append(tap_ok)
        conv_out = conv_out + conv_w[offset] * jnp.where(tap_ok, u_shift, 0.0)
    reset = jnp.logical_not(mask_list[1])
    conv_bf = conv_out.astype(jnp.bfloat16).astype(jnp.float32).reshape(SEQ, HEADS, BLOCK_W)
    wa_full = a_gate_w.astype(jnp.float32)
    wi_full = x_gate_w.astype(jnp.float32)
    pre_a = jnp.einsum('thk,hkj->thj', conv_bf, wa_full).reshape(SEQ, D_RNN) + a_gate_b
    pre_i = jnp.einsum('thk,hkj->thj', conv_bf, wi_full).reshape(SEQ, D_RNN) + x_gate_b

    def lru_of(conv_v, pre_av, pre_iv, lam_v):
        return lru_scan(conv_v, pre_av, pre_iv, lam_v, reset)

    _, vjp_fn = jax.vjp(lru_of, conv_out, pre_a, pre_i, lam_param)
    d_conv, d_pre_a, d_pre_i, d_lam = vjp_fn(grad_row)
    ga_bf = d_pre_a.astype(jnp.bfloat16).astype(jnp.float32).reshape(SEQ, HEADS, BLOCK_W)
    gi_bf = d_pre_i.astype(jnp.bfloat16).astype(jnp.float32).reshape(SEQ, HEADS, BLOCK_W)
    back_gates = jnp.einsum('thj,hkj->thk', ga_bf, wa_full) + jnp.einsum('thj,hkj->thk', gi_bf, wi_full)
    d_conv = d_conv + back_gates.reshape(SEQ, D_RNN)
    g_wa = jnp.einsum('thk,thj->hkj', conv_bf, ga_bf)
    g_wi = jnp.einsum('thk,thj->hkj', conv_bf, gi_bf)
    du_row = jnp.zeros_like(d_conv)
    g_w_list = []
    for offset in range(CONV):
        masked = jnp.where(mask_list[offset], d_conv, 0.0)
        du_row = du_row + conv_w[offset] * jnp.pad(masked, ((0, offset), (0, 0)))[offset:]
        u_shift = jnp.pad(u_row, ((offset, 0), (0, 0)))[:SEQ].astype(jnp.float32)
        g_w_list.append(jnp.sum(masked * u_shift, axis=0))
    grads = (jnp.stack(g_w_list), jnp.sum(d_conv, axis=0), g_wa, jnp.sum(d_pre_a, axis=0),
             g_wi, jnp.sum(d_pre_i, axis=0), d_lam)
    return du_row.astype(jnp.bfloat16), grads


def reference(u_in, seg_ids, grad_h, conv_w, conv_b, a_gate_w, a_gate_b, x_gate_w, x_gate_b, lam_param):
    def per_row(row_in):
        u_row, seg_row, grad_row = row_in
        return row_grads(u_row, seg_row, grad_row, conv_w, conv_b, a_gate_w, a_gate_b,
                         x_gate_w, x_gate_b, lam_param)

    grad_u, row_parts = lax.map(per_row, (u_in, seg_ids, grad_h))
    totals = [jnp.sum(piece, axis=0) for piece in row_parts]
    return (grad_u, totals[0], totals[1], totals[2], totals[3], totals[4], totals[5], totals[6])
```

```python
import functools

import jax
import jax.numpy as jnp
from jax import lax
from jax.experimental import pallas as pl
from jax.experimental.pallas import tpu as pltpu
from jax.sharding import PartitionSpec as P

CONV = 4
HALO = CONV - 1
LOG2E = 1.4426950408889634
LANES = 128
STEPS = 8

W0, BC, BA, BI, KL, KE = 0, 4, 5, 6, 7, 8
N_PAR = 16
GW, GBC, GBA, GBI, GLAM = 0, 4, 5, 6, 7
N_VEC = 8


def sigmoid_of(pre):
    root = lax.rsqrt(1.0 + jnp.exp2(pre * (-LOG2E)))
    return root * root


def decay_of(gate_r, par_kl, par_ke, keep):
    a_raw = jnp.exp2(gate_r * par_ke)
    gap = jnp.tanh(gate_r * (-par_kl)) * (1.0 + a_raw * a_raw)
    inv_root = lax.rsqrt(gap)
    decay = a_raw * keep
    mult = jnp.where(keep > 0.5, gap * inv_root, 1.0)
    return decay, mult, decay * decay * inv_root


def fold_rows(arr):
    return arr[:8] + arr[8:]


def dot_nn(lhs, rhs):
    return lax.dot_general(lhs, rhs, (((1,), (0,)), ((), ())), preferred_element_type=jnp.float32)


def dot_nt(lhs, rhs):
    return lax.dot_general(lhs, rhs, (((1,), (1,)), ((), ())), preferred_element_type=jnp.float32)


def dot_tn(lhs, rhs):
    return lax.dot_general(lhs, rhs, (((0,), (0,)), ((), ())), preferred_element_type=jnp.float32)


def load_u(u_ref, halo_ref, u_scr):
    n_tok = u_ref.shape[1]
    u_scr[:HALO] = halo_ref[...]
    for start in range(0, n_tok, 16):
        u_scr[HALO + start:HALO + start + 16] = jnp.swapaxes(u_ref[:, start:start + 16, :].astype(jnp.float32), 0, 1)


def first_kernel(u_ref, gh_ref, halo_ref, mask_ref, wa_ref, wi_ref, par_ref,
                 sum_ref, c_ref, r_ref, i_ref, u_scr, cb_scr, pa_scr, pi_scr, a_scr, g_scr):
    n_batch, n_tok, width = u_ref.shape
    load_u(u_ref, halo_ref, u_scr)

    def conv_body(chunk, _):
        base = chunk * STEPS
        for step in range(STEPS):
            tok = base + step
            for lane in range(0, width, LANES):
                cols = slice(lane, lane + LANES)
                acc = par_ref[BC:BC + 1, cols] + par_ref[W0:W0 + 1, cols] * u_scr[tok + HALO, :, cols]
                for tap in range(1, CONV):
                    acc = acc + par_ref[W0 + tap:W0 + tap + 1, cols] * (mask_ref[tap - 1, tok] * u_scr[tok + HALO - tap, :, cols])
                c_ref[tok, :, cols] = acc
                cb_scr[tok, :, cols] = acc.astype(jnp.bfloat16)
        return 0

    lax.fori_loop(0, n_tok // STEPS, conv_body, 0)
    rows = 256
    for start in range(0, n_tok, rows // n_batch):
        toks = slice(start, start + rows // n_batch)
        part = cb_scr[toks].reshape(rows, width)
        pa_scr[toks] = dot_nn(part, wa_ref[0]).reshape(rows // n_batch, n_batch, width)
        pi_scr[toks] = dot_nn(part, wi_ref[0]).reshape(rows // n_batch, n_batch, width)

    for start in range(0, n_tok, 8):
        g_scr[start:start + 8] = jnp.swapaxes(gh_ref[:, start:start + 8, :], 0, 1)

    for lane in range(0, width, LANES):
        cols = slice(lane, lane + LANES)

        def fwd_body(chunk, carry):
            state, prod = carry
            base = chunk * STEPS
            for step in range(STEPS):
                tok = base + step
                gate_r = sigmoid_of(pa_scr[tok, :, cols] + par_ref[BA:BA + 1, cols])
                gate_i = sigmoid_of(pi_scr[tok, :, cols] + par_ref[BI:BI + 1, cols])
                decay, mult, _ = decay_of(gate_r, par_ref[KL:KL + 1, cols], par_ref[KE:KE + 1, cols], mask_ref[0, tok])
                r_ref[tok, :, cols] = gate_r
                i_ref[tok, :, cols] = gate_i
                a_scr[tok, :, cols] = decay
                state = decay * state + mult * (gate_i * c_ref[tok, :, cols])
                prod = decay * prod
            return state, prod

        zero = jnp.zeros((n_batch, LANES), jnp.float32)
        state, prod = lax.fori_loop(0, n_tok // STEPS, fwd_body, (zero, zero + 1.0))
        sum_ref[0, :, cols] = prod
        sum_ref[1, :, cols] = state

        def bwd_body(chunk, adj):
            base = n_tok - STEPS - chunk * STEPS
            for step in reversed(range(STEPS)):
                tok = base + step
                adj = a_scr[tok, :, cols] * (g_scr[tok, :, cols] + adj)
            return adj

        sum_ref[2, :, cols] = lax.fori_loop(0, n_tok // STEPS, bwd_body, zero)


def second_kernel(u_ref, gh_ref, halo_ref, mask_ref, wa_ref, wi_ref, par_ref, c_ref, r_ref, i_ref, in_ref,
                  du_ref, tail_ref, back_ref, dwa_ref, dwi_ref, vec_ref,
                  u_scr, cb_scr, ga_scr, gi_scr, a_scr, m_scr, e_scr, h_scr, d_scr, g_scr):
    n_batch, n_tok, width = u_ref.shape
    load_u(u_ref, halo_ref, u_scr)
    for start in range(0, n_tok, 8):
        g_scr[start:start + 8] = jnp.swapaxes(gh_ref[:, start:start + 8, :], 0, 1)

    for lane in range(0, width, LANES):
        cols = slice(lane, lane + LANES)
        zero8 = jnp.zeros((8, LANES), jnp.float32)

        def fwd_body(chunk, state):
            base = chunk * STEPS
            for step in range(STEPS):
                tok = base + step
                conv_c = c_ref[tok, :, cols]
                decay, mult, ratio = decay_of(r_ref[tok, :, cols], par_ref[KL:KL + 1, cols], par_ref[KE:KE + 1, cols], mask_ref[0, tok])
                a_scr[tok, :, cols] = decay
                m_scr[tok, :, cols] = mult
                e_scr[tok, :, cols] = ratio
                h_scr[tok, :, cols] = state
                cb_scr[tok, :, cols] = conv_c.astype(jnp.bfloat16)
                state = decay * state + mult * (i_ref[tok, :, cols] * conv_c)
            return state

        lax.fori_loop(0, n_tok // STEPS, fwd_body, in_ref[0, :, cols])

        def bwd_body(chunk, carry):
            adj_next, sum_a, sum_i, sum_l = carry
            base = n_tok - STEPS - chunk * STEPS
            for step in reversed(range(STEPS)):
                tok = base + step
                gate_r = r_ref[tok, :, cols]
                gate_i = i_ref[tok, :, cols]
                conv_c = c_ref[tok, :, cols]
                adj = g_scr[tok, :, cols] + adj_next
                adj_next = a_scr[tok, :, cols] * adj
                d_log = adj_next * h_scr[tok, :, cols] - adj * (gate_i * conv_c) * e_scr[tok, :, cols]
                direct = adj * m_scr[tok, :, cols] * gate_i
                d_pre_i = direct * conv_c * (1.0 - gate_i)
                d_log_r = d_log * gate_r
                d_pre_a = d_log_r * (par_ref[KL:KL + 1, cols] * (1.0 - gate_r))
                sum_l = sum_l + fold_rows(d_log_r)
                sum_a = sum_a + fold_rows(d_pre_a)
                sum_i = sum_i + fold_rows(d_pre_i)
                d_scr[tok, :, cols] = direct
                ga_scr[tok, :, cols] = d_pre_a.astype(jnp.bfloat16)
                gi_scr[tok, :, cols] = d_pre_i.astype(jnp.bfloat16)
            return adj_next, sum_a, sum_i, sum_l

        _, sum_a, sum_i, sum_l = lax.fori_loop(0, n_tok // STEPS, bwd_body, (in_ref[1, :, cols], zero8, zero8, zero8))
        vec_ref[0, GBA:GBA + 1, cols] = jnp.sum(sum_a, axis=0, keepdims=True)
        vec_ref[0, GBI:GBI + 1, cols] = jnp.sum(sum_i, axis=0, keepdims=True)
        vec_ref[0, GLAM:GLAM + 1, cols] = jnp.sum(sum_l, axis=0, keepdims=True)

    rows = 256
    for start in range(0, n_tok, rows // n_batch):
        toks = slice(start, start + rows // n_batch)
        back = dot_nt(ga_scr[toks].reshape(rows, width), wa_ref[0]) + dot_nt(gi_scr[toks].reshape(rows, width), wi_ref[0])
        d_scr[toks] = d_scr[toks] + back.reshape(rows // n_batch, n_batch, width)
    all_c = cb_scr[...].reshape(n_tok * n_batch, width)
    dwa_ref[0] = dot_tn(all_c, ga_scr[...].reshape(n_tok * n_batch, width))
    dwi_ref[0] = dot_tn(all_c, gi_scr[...].reshape(n_tok * n_batch, width))

    for lane in range(0, width, LANES):
        cols = slice(lane, lane + LANES)
        zero8 = jnp.zeros((8, LANES), jnp.float32)
        zero = jnp.zeros((n_batch, LANES), jnp.float32)

        def tap_body(chunk, carry):
            sums = list(carry[:CONV + 1])
            ahead = list(carry[CONV + 1:])
            base = n_tok - STEPS - chunk * STEPS
            for step in reversed(range(STEPS)):
                tok = base + step
                d_conv = d_scr[tok, :, cols]
                sums[CONV] = sums[CONV] + fold_rows(d_conv)
                masked = [d_conv] + [mask_ref[tap - 1, tok] * d_conv for tap in range(1, CONV)]
                for tap in range(CONV):
                    sums[tap] = sums[tap] + fold_rows(masked[tap] * u_scr[tok + HALO - tap, :, cols])
                terms = [par_ref[W0 + tap:W0 + tap + 1, cols] * masked[tap] for tap in range(CONV)]
                a_scr[tok, :, cols] = ahead[0] + terms[0]
                ahead = [ahead[1] + terms[1], ahead[2] + terms[2], terms[3]]
            return tuple(sums) + tuple(ahead)

        out = lax.fori_loop(0, n_tok // STEPS, tap_body, (zero8,) * (CONV + 1) + (zero,) * HALO)
        for row in range(CONV + 1):
            vec_ref[0, GW + row:GW + row + 1, cols] = jnp.sum(out[row], axis=0, keepdims=True)
        for row in range(HALO):
            back_ref[HALO - 1 - row, :, cols] = out[CONV + 1 + row]

    tail_ref[...] = a_scr[n_tok - HALO:]
    for start in range(0, n_tok, 16):
        du_ref[:, start:start + 16, :] = jnp.swapaxes(a_scr[start:start + 16], 0, 1).astype(jnp.bfloat16)


def solution(mesh):
    n_dev = mesh.shape['cp']
    to_next = [(src, src + 1) for src in range(n_dev - 1)]
    to_prev = [(src + 1, src) for src in range(n_dev - 1)]
    seq_spec = P(None, 'cp', None)
    rep_spec = P()

    def local_fn(u_in, seg_ids, grad_h, conv_w, conv_b, a_gate_w, a_gate_b, x_gate_w, x_gate_b, lam_param):
        n_batch, n_tok, n_width = u_in.shape
        n_heads, block_w, _ = a_gate_w.shape
        has_prev = lax.axis_index('cp') > 0
        tail_pack = jnp.concatenate([u_in[:, n_tok - HALO:, :].astype(jnp.float32),
                                     seg_ids[:, n_tok - HALO:, None].astype(jnp.float32)], axis=2)
        recv_pack = lax.ppermute(tail_pack, 'cp', to_next)
        halo_u = jnp.swapaxes(recv_pack[:, :, :n_width], 0, 1)
        halo_seg = recv_pack[:, :, n_width].astype(jnp.int32)
        seg_ext = jnp.concatenate([halo_seg, seg_ids], axis=1).T
        ext_ok = (jnp.arange(n_tok + HALO) >= HALO) | has_prev
        masks = []
        for tap in range(1, CONV):
            tap_ok = (seg_ext[HALO - tap:HALO - tap + n_tok] == seg_ext[HALO:]) & ext_ok[HALO - tap:HALO - tap + n_tok, None]
            masks.append(tap_ok.astype(jnp.float32))
        masks = jnp.broadcast_to(jnp.stack(masks)[..., None], (HALO, n_tok, n_batch, LANES))
        log_rate = -8.0 * jax.nn.softplus(-lam_param)
        par = jnp.concatenate([conv_w, conv_b[None], a_gate_b[None], x_gate_b[None], log_rate[None], log_rate[None] * LOG2E,
                               jnp.zeros((N_PAR - 9, n_width), jnp.float32)], axis=0)

        def blk_row():
            return pl.BlockSpec((n_batch, n_tok, block_w), lambda h: (0, 0, h))

        def blk_time(count):
            return pl.BlockSpec((count, n_batch, block_w), lambda h: (0, 0, h))

        mask_spec = pl.BlockSpec((HALO, n_tok, n_batch, LANES), lambda h: (0, 0, 0, 0))
        mat_spec = pl.BlockSpec((1, block_w, block_w), lambda h: (h, 0, 0))
        par_spec = pl.BlockSpec((N_PAR, block_w), lambda h: (0, h))
        save_spec = pl.BlockSpec((None, n_tok, n_batch, block_w), lambda h: (h, 0, 0, 0))
        save_shape = jax.ShapeDtypeStruct((n_heads, n_tok, n_batch, block_w), jnp.float32)
        f32_scr = pltpu.VMEM((n_tok, n_batch, block_w), jnp.float32)
        bf_scr = pltpu.VMEM((n_tok, n_batch, block_w), jnp.bfloat16)
        u_scr = pltpu.VMEM((n_tok + HALO, n_batch, block_w), jnp.float32)
        limit = pltpu.CompilerParams(vmem_limit_bytes=60 * 2 ** 20)

        sums, sav_c, sav_r, sav_i = pl.pallas_call(
            first_kernel, grid=(n_heads,),
            in_specs=[blk_row(), blk_row(), blk_time(HALO), mask_spec, mat_spec, mat_spec, par_spec],
            out_specs=[blk_time(3), save_spec, save_spec, save_spec],
            out_shape=[jax.ShapeDtypeStruct((3, n_batch, n_width), jnp.float32), save_shape, save_shape, save_shape],
            scratch_shapes=[u_scr, bf_scr, f32_scr, f32_scr, f32_scr, f32_scr],
            compiler_params=limit, name='local_pass',
        )(u_in, grad_h, halo_u, masks, a_gate_w, x_gate_w, par)

        half = n_width * n_batch // n_dev
        mine = lax.all_to_all(sums.reshape(3, n_dev, half), 'cp', split_axis=1, concat_axis=1, tiled=True)
        prods, states, firsts = mine[0], mine[1], mine[2]
        into_state = [jnp.zeros((half,), jnp.float32)]
        for dev in range(n_dev - 1):
            into_state.append(prods[dev] * into_state[-1] + states[dev])
        into_adj = [jnp.zeros((half,), jnp.float32)]
        for dev in range(n_dev - 1, 0, -1):
            into_adj.append(prods[dev] * into_adj[-1] + firsts[dev])
        give = jnp.stack([jnp.stack(into_state), jnp.stack(into_adj[::-1])])
        carry_in = lax.all_to_all(give, 'cp', split_axis=1, concat_axis=1, tiled=True).reshape(2, n_batch, n_width)

        grad_u, tail, back, g_wa, g_wi, vecs = pl.pallas_call(
            second_kernel, grid=(n_heads,),
            in_specs=[blk_row(), blk_row(), blk_time(HALO), mask_spec, mat_spec, mat_spec, par_spec,
                      save_spec, save_spec, save_spec, blk_time(2)],
            out_specs=[blk_row(), blk_time(HALO), blk_time(HALO), mat_spec, mat_spec, pl.BlockSpec((1, N_VEC, block_w), lambda h: (h, 0, 0))],
            out_shape=[jax.ShapeDtypeStruct(u_in.shape, jnp.bfloat16), jax.ShapeDtypeStruct((HALO, n_batch, n_width), jnp.float32),
                       jax.ShapeDtypeStruct((HALO, n_batch, n_width), jnp.float32),
                       jax.ShapeDtypeStruct(a_gate_w.shape, jnp.float32), jax.ShapeDtypeStruct(a_gate_w.shape, jnp.float32),
                       jax.ShapeDtypeStruct((n_heads, N_VEC, block_w), jnp.float32)],
            scratch_shapes=[u_scr, bf_scr, bf_scr, bf_scr] + [f32_scr] * 6,
            compiler_params=limit, name='full_pass',
        )(u_in, grad_h, halo_u, masks, a_gate_w, x_gate_w, par, sav_c, sav_r, sav_i, carry_in)
        halo_back = lax.ppermute(back, 'cp', to_prev)
        return grad_u, tail, halo_back, g_wa, g_wi, vecs

    def full_fn(*args):
        lam_param = args[-1]
        grad_u, tail, halo_back, g_wa, g_wi, vecs = local_fn(*args)
        tail = jnp.swapaxes((tail + halo_back).astype(jnp.bfloat16), 0, 1)
        grad_u = lax.dynamic_update_slice(grad_u, tail, (0, grad_u.shape[1] - HALO, 0))
        g_wa, g_wi, vecs = lax.psum((g_wa, g_wi, vecs), 'cp')
        vecs = jnp.swapaxes(vecs, 0, 1).reshape(N_VEC, -1)
        g_lam = 8.0 * jax.nn.sigmoid(-lam_param) * vecs[GLAM]
        return (grad_u, vecs[GW:GW + CONV], vecs[GBC], g_wa, vecs[GBA], g_wi, vecs[GBI], g_lam)

    return jax.shard_map(full_fn, mesh=mesh,
                         in_specs=(seq_spec, P(None, 'cp'), seq_spec, rep_spec, rep_spec, rep_spec,
                                   rep_spec, rep_spec, rep_spec, rep_spec),
                         out_specs=(seq_spec,) + (rep_spec,) * 7, check_vma=False)
```

```python
import functools

import jax
import jax.numpy as jnp
from jax import lax
from jax.experimental import pallas as pl
from jax.experimental.pallas import tpu as pltpu
from jax.sharding import PartitionSpec as P

CONV = 4
HALO = CONV - 1
LOG2E = 1.4426950408889634
LANES = 128
STEPS = 8
LAG = 2
SLOTS = LAG + 1
ROWS = 8

W0, BC, BA, BI, KL, KE = 0, 4, 5, 6, 7, 8
N_PAR = 16
GW, GBC, GBA, GBI, GLAM = 0, 4, 5, 6, 7
N_VEC = 8


def sigmoid_of(pre):
    root = lax.rsqrt(1.0 + jnp.exp2(pre * (-LOG2E)))
    return root * root


def decay_of(gate_r, par_kl, par_ke, keep):
    a_raw = jnp.exp2(gate_r * par_ke)
    gap = jnp.tanh(gate_r * (-par_kl)) * (1.0 + a_raw * a_raw)
    inv_root = lax.rsqrt(gap)
    decay = a_raw * keep
    mult = jnp.where(keep > 0.5, gap * inv_root, 1.0)
    return decay, mult, decay * decay * inv_root


def fold_rows(arr):
    return arr[:8] + arr[8:]


def dot_nn(lhs, rhs):
    return lax.dot_general(lhs, rhs, (((1,), (0,)), ((), ())), preferred_element_type=jnp.float32)


def dot_nt(lhs, rhs):
    return lax.dot_general(lhs, rhs, (((1,), (1,)), ((), ())), preferred_element_type=jnp.float32)


def dot_tn(lhs, rhs):
    return lax.dot_general(lhs, rhs, (((0,), (0,)), ((), ())), preferred_element_type=jnp.float32)


def fused_kernel(n_dev, n_heads,
                 u_ref, gh_ref, halo_ref, mask_ref, wa_ref, wi_ref, wa2_ref, wi2_ref, par_ref, par2_ref,
                 du_ref, tail_ref, back_ref, dwa_ref, dwi_ref, vec_ref,
                 u_s, c_s, r_s, i_s, a_s, m_s, e_s, g_s, cb_s, h_scr, d_scr, ga_scr, gi_scr,
                 send, recv, resp, carry, send_sem, recv_sem, give_sem, take_sem):
    n_batch, n_tok, width = u_ref.shape
    step_id = pl.program_id(0)
    me = lax.axis_index('cp')
    rows = 256
    span = rows // n_batch

    def spread(src, dst, out_sem, in_sem, head, count):
        def one(k, _):
            dev = lax.rem(me + k, n_dev)
            pltpu.make_async_remote_copy(
                src_ref=src.at[head, pl.ds(pl.multiple_of(dev * ROWS, ROWS), count)],
                dst_ref=dst.at[head, pl.ds(pl.multiple_of(me * ROWS, ROWS), count)],
                send_sem=out_sem.at[head], recv_sem=in_sem.at[head],
                device_id=(dev,), device_id_type=pl.DeviceIdType.MESH).start()
            return 0
        lax.fori_loop(1, n_dev, one, 0)
        own = pl.ds(pl.multiple_of(me * ROWS, ROWS), ROWS)
        dst[head, own, :] = src[head, own, :]

    def settle(buf, sem, head, count):
        total = buf.at[head, pl.ds(0, (n_dev - 1) * count)]
        pltpu.make_async_copy(total, total, sem.at[head]).wait()

    @pl.when((step_id >= 1) & (step_id <= n_heads))
    def _combine():
        head = step_id - 1
        settle(recv, recv_sem, head, 3)
        state = jnp.zeros((1, LANES), jnp.float32)
        adj = jnp.zeros((1, LANES), jnp.float32)
        for dev in range(n_dev):
            row, back_row = dev * ROWS, (n_dev - 1 - dev) * ROWS
            resp[head, row:row + 1, :] = state
            resp[head, back_row + 1:back_row + 2, :] = adj
            state = recv[head, row:row + 1, :] * state + recv[head, row + 1:row + 2, :]
            adj = recv[head, back_row:back_row + 1, :] * adj + recv[head, back_row + 2:back_row + 3, :]
        spread(resp, carry, give_sem, take_sem, head, 2)

    @pl.when(step_id < n_heads)
    def _first():
        head = step_id
        slot = lax.rem(step_id, SLOTS)
        u_s[slot, :HALO] = halo_ref[...]
        for start in range(0, n_tok, 16):
            u_s[slot, HALO + start:HALO + start + 16] = jnp.swapaxes(u_ref[:, start:start + 16, :].astype(jnp.float32), 0, 1)
        for start in range(0, n_tok, 8):
            g_s[slot, start:start + 8] = jnp.swapaxes(gh_ref[:, start:start + 8, :], 0, 1)

        def conv_body(chunk, _):
            base = chunk * STEPS
            for step in range(STEPS):
                tok = base + step
                for lane in range(0, width, LANES):
                    cols = slice(lane, lane + LANES)
                    acc = par_ref[BC:BC + 1, cols] + par_ref[W0:W0 + 1, cols] * u_s[slot, tok + HALO, :, cols]
                    for tap in range(1, CONV):
                        acc = acc + par_ref[W0 + tap:W0 + tap + 1, cols] * (mask_ref[tap - 1, tok] * u_s[slot, tok + HALO - tap, :, cols])
                    c_s[slot, tok, :, cols] = acc
                    cb_s[slot, tok, :, cols] = acc.astype(jnp.bfloat16)
            return 0

        lax.fori_loop(0, n_tok // STEPS, conv_body, 0)
        for start in range(0, n_tok, span):
            part = cb_s[slot, start:start + span].reshape(rows, width)
            r_s[slot, start:start + span] = dot_nn(part, wa_ref[0]).reshape(span, n_batch, width)
            i_s[slot, start:start + span] = dot_nn(part, wi_ref[0]).reshape(span, n_batch, width)

        for half in range(width // LANES):
            cols = slice(half * LANES, (half + 1) * LANES)

            def fwd_body(chunk, run):
                state, prod = run
                base = chunk * STEPS
                for step in range(STEPS):
                    tok = base + step
                    gate_r = sigmoid_of(r_s[slot, tok, :, cols] + par_ref[BA:BA + 1, cols])
                    gate_i = sigmoid_of(i_s[slot, tok, :, cols] + par_ref[BI:BI + 1, cols])
                    decay, mult, ratio = decay_of(gate_r, par_ref[KL:KL + 1, cols], par_ref[KE:KE + 1, cols], mask_ref[0, tok])
                    r_s[slot, tok, :, cols] = gate_r
                    i_s[slot, tok, :, cols] = gate_i
                    a_s[slot, tok, :, cols] = decay
                    m_s[slot, tok, :, cols] = mult
                    e_s[slot, tok, :, cols] = ratio
                    state = decay * state + mult * (gate_i * c_s[slot, tok, :, cols])
                    prod = decay * prod
                return state, prod

            zero = jnp.zeros((n_batch, LANES), jnp.float32)
            state, prod = lax.fori_loop(0, n_tok // STEPS, fwd_body, (zero, zero + 1.0))

            def adj_body(chunk, adj):
                base = n_tok - STEPS - chunk * STEPS
                for step in reversed(range(STEPS)):
                    tok = base + step
                    adj = a_s[slot, tok, :, cols] * (g_s[slot, tok, :, cols] + adj)
                return adj

            first = lax.fori_loop(0, n_tok // STEPS, adj_body, zero)
            for row, val in enumerate((prod, state, first)):
                send.at[head][pl.ds(half * ROWS + row, n_batch, stride=2 * ROWS), :] = val
        spread(send, recv, send_sem, recv_sem, head, 3)

    @pl.when(step_id >= LAG)
    def _second():
        head = step_id - LAG
        slot = lax.rem(step_id - LAG, SLOTS)
        settle(carry, take_sem, head, 2)

        for half in range(width // LANES):
            cols = slice(half * LANES, (half + 1) * LANES)
            zero8 = jnp.zeros((8, LANES), jnp.float32)

            def fwd_body(chunk, state):
                base = chunk * STEPS
                for step in range(STEPS):
                    tok = base + step
                    h_scr[tok, :, cols] = state
                    state = a_s[slot, tok, :, cols] * state + m_s[slot, tok, :, cols] * (i_s[slot, tok, :, cols] * c_s[slot, tok, :, cols])
                return state

            lax.fori_loop(0, n_tok // STEPS, fwd_body, carry.at[head][pl.ds(half * ROWS, n_batch, stride=2 * ROWS), :])

            def bwd_body(chunk, run):
                adj_next, sum_a, sum_i, sum_l = run
                base = n_tok - STEPS - chunk * STEPS
                for step in reversed(range(STEPS)):
                    tok = base + step
                    gate_r = r_s[slot, tok, :, cols]
                    gate_i = i_s[slot, tok, :, cols]
                    conv_c = c_s[slot, tok, :, cols]
                    adj = g_s[slot, tok, :, cols] + adj_next
                    adj_next = a_s[slot, tok, :, cols] * adj
                    d_log = adj_next * h_scr[tok, :, cols] - adj * (gate_i * conv_c) * e_s[slot, tok, :, cols]
                    direct = adj * m_s[slot, tok, :, cols] * gate_i
                    d_pre_i = direct * conv_c * (1.0 - gate_i)
                    d_log_r = d_log * gate_r
                    d_pre_a = d_log_r * (par2_ref[KL:KL + 1, cols] * (1.0 - gate_r))
                    sum_l = sum_l + fold_rows(d_log_r)
                    sum_a = sum_a + fold_rows(d_pre_a)
                    sum_i = sum_i + fold_rows(d_pre_i)
                    d_scr[tok, :, cols] = direct
                    ga_scr[tok, :, cols] = d_pre_a.astype(jnp.bfloat16)
                    gi_scr[tok, :, cols] = d_pre_i.astype(jnp.bfloat16)
                return adj_next, sum_a, sum_i, sum_l

            adj_in = carry.at[head][pl.ds(half * ROWS + 1, n_batch, stride=2 * ROWS), :]
            _, sum_a, sum_i, sum_l = lax.fori_loop(0, n_tok // STEPS, bwd_body, (adj_in, zero8, zero8, zero8))
            vec_ref[0, GBA:GBA + 1, cols] = jnp.sum(sum_a, axis=0, keepdims=True)
            vec_ref[0, GBI:GBI + 1, cols] = jnp.sum(sum_i, axis=0, keepdims=True)
            vec_ref[0, GLAM:GLAM + 1, cols] = jnp.sum(sum_l, axis=0, keepdims=True)

        for start in range(0, n_tok, span):
            toks = slice(start, start + span)
            back = dot_nt(ga_scr[toks].reshape(rows, width), wa2_ref[0]) + dot_nt(gi_scr[toks].reshape(rows, width), wi2_ref[0])
            d_scr[toks] = d_scr[toks] + back.reshape(span, n_batch, width)
        all_c = cb_s[slot].reshape(n_tok * n_batch, width)
        dwa_ref[0] = dot_tn(all_c, ga_scr[...].reshape(n_tok * n_batch, width))
        dwi_ref[0] = dot_tn(all_c, gi_scr[...].reshape(n_tok * n_batch, width))

        for half in range(width // LANES):
            cols = slice(half * LANES, (half + 1) * LANES)
            zero8 = jnp.zeros((8, LANES), jnp.float32)
            zero = jnp.zeros((n_batch, LANES), jnp.float32)

            def tap_body(chunk, run):
                sums = list(run[:CONV + 1])
                ahead = list(run[CONV + 1:])
                base = n_tok - STEPS - chunk * STEPS
                for step in reversed(range(STEPS)):
                    tok = base + step
                    d_conv = d_scr[tok, :, cols]
                    sums[CONV] = sums[CONV] + fold_rows(d_conv)
                    masked = [d_conv] + [mask_ref[tap - 1, tok] * d_conv for tap in range(1, CONV)]
                    for tap in range(CONV):
                        sums[tap] = sums[tap] + fold_rows(masked[tap] * u_s[slot, tok + HALO - tap, :, cols])
                    terms = [par2_ref[W0 + tap:W0 + tap + 1, cols] * masked[tap] for tap in range(CONV)]
                    h_scr[tok, :, cols] = ahead[0] + terms[0]
                    ahead = [ahead[1] + terms[1], ahead[2] + terms[2], terms[3]]
                return tuple(sums) + tuple(ahead)

            out = lax.fori_loop(0, n_tok // STEPS, tap_body, (zero8,) * (CONV + 1) + (zero,) * HALO)
            for row in range(CONV + 1):
                vec_ref[0, GW + row:GW + row + 1, cols] = jnp.sum(out[row], axis=0, keepdims=True)
            for row in range(HALO):
                back_ref[HALO - 1 - row, :, cols] = out[CONV + 1 + row]

        tail_ref[...] = h_scr[n_tok - HALO:]
        for start in range(0, n_tok, 16):
            du_ref[:, start:start + 16, :] = jnp.swapaxes(h_scr[start:start + 16], 0, 1).astype(jnp.bfloat16)

    @pl.when(step_id == n_heads - 1 + LAG)
    def _drain():
        def one(head, _):
            settle(send, send_sem, head, 3)
            settle(resp, give_sem, head, 2)
            return 0
        lax.fori_loop(0, n_heads, one, 0)


def solution(mesh):
    n_dev = mesh.shape['cp']
    to_next = [(src, src + 1) for src in range(n_dev - 1)]
    to_prev = [(src + 1, src) for src in range(n_dev - 1)]
    seq_spec = P(None, 'cp', None)
    rep_spec = P()

    def local_fn(u_in, seg_ids, grad_h, conv_w, conv_b, a_gate_w, a_gate_b, x_gate_w, x_gate_b, lam_param):
        n_batch, n_tok, n_width = u_in.shape
        n_heads, block_w, _ = a_gate_w.shape
        has_prev = lax.axis_index('cp') > 0
        tail_pack = jnp.concatenate([u_in[:, n_tok - HALO:, :].astype(jnp.float32),
                                     seg_ids[:, n_tok - HALO:, None].astype(jnp.float32)], axis=2)
        recv_pack = lax.ppermute(tail_pack, 'cp', to_next)
        halo_u = jnp.swapaxes(recv_pack[:, :, :n_width], 0, 1)
        halo_seg = recv_pack[:, :, n_width].astype(jnp.int32)
        seg_ext = jnp.concatenate([halo_seg, seg_ids], axis=1).T
        ext_ok = (jnp.arange(n_tok + HALO) >= HALO) | has_prev
        masks = []
        for tap in range(1, CONV):
            tap_ok = (seg_ext[HALO - tap:HALO - tap + n_tok] == seg_ext[HALO:]) & ext_ok[HALO - tap:HALO - tap + n_tok, None]
            masks.append(tap_ok.astype(jnp.float32))
        masks = jnp.broadcast_to(jnp.stack(masks)[..., None], (HALO, n_tok, n_batch, LANES))
        log_rate = -8.0 * jax.nn.softplus(-lam_param)
        par = jnp.concatenate([conv_w, conv_b[None], a_gate_b[None], x_gate_b[None], log_rate[None], log_rate[None] * LOG2E,
                               jnp.zeros((N_PAR - 9, n_width), jnp.float32)], axis=0)

        def now(step):
            return jnp.minimum(step, n_heads - 1)

        def late(step):
            return jnp.maximum(step - LAG, 0)

        def blk_row(at):
            return pl.BlockSpec((n_batch, n_tok, block_w), lambda s: (0, 0, at(s)))

        def blk_time(count, at):
            return pl.BlockSpec((count, n_batch, block_w), lambda s: (0, 0, at(s)))

        def mat_spec(at):
            return pl.BlockSpec((1, block_w, block_w), lambda s: (at(s), 0, 0))

        def par_spec(at):
            return pl.BlockSpec((N_PAR, block_w), lambda s: (0, at(s)))

        mask_spec = pl.BlockSpec((HALO, n_tok, n_batch, LANES), lambda s: (0, 0, 0, 0))
        f32_slots = pltpu.VMEM((SLOTS, n_tok, n_batch, block_w), jnp.float32)
        f32_scr = pltpu.VMEM((n_tok, n_batch, block_w), jnp.float32)
        bf_scr = pltpu.VMEM((n_tok, n_batch, block_w), jnp.bfloat16)
        wire = pltpu.VMEM((n_heads, n_dev * ROWS, LANES), jnp.float32)
        sems = pltpu.SemaphoreType.DMA((n_heads,))

        grad_u, tail, back, g_wa, g_wi, vecs = pl.pallas_call(
            functools.partial(fused_kernel, n_dev, n_heads), grid=(n_heads + LAG,),
            in_specs=[blk_row(now), blk_row(now), blk_time(HALO, now), mask_spec, mat_spec(now), mat_spec(now),
                      mat_spec(late), mat_spec(late), par_spec(now), par_spec(late)],
            out_specs=[blk_row(late), blk_time(HALO, late), blk_time(HALO, late), mat_spec(late), mat_spec(late),
                       pl.BlockSpec((1, N_VEC, block_w), lambda s: (late(s), 0, 0))],
            out_shape=[jax.ShapeDtypeStruct(u_in.shape, jnp.bfloat16), jax.ShapeDtypeStruct((HALO, n_batch, n_width), jnp.float32),
                       jax.ShapeDtypeStruct((HALO, n_batch, n_width), jnp.float32),
                       jax.ShapeDtypeStruct(a_gate_w.shape, jnp.float32), jax.ShapeDtypeStruct(a_gate_w.shape, jnp.float32),
                       jax.ShapeDtypeStruct((n_heads, N_VEC, block_w), jnp.float32)],
            scratch_shapes=[pltpu.VMEM((SLOTS, n_tok + HALO, n_batch, block_w), jnp.float32)] + [f32_slots] * 7
            + [pltpu.VMEM((SLOTS, n_tok, n_batch, block_w), jnp.bfloat16), f32_scr, f32_scr, bf_scr, bf_scr]
            + [wire] * 4 + [sems] * 4,
            compiler_params=pltpu.CompilerParams(vmem_limit_bytes=63 * 2 ** 20, has_side_effects=True), name='fused_pass',
        )(u_in, grad_h, halo_u, masks, a_gate_w, x_gate_w, a_gate_w, x_gate_w, par, par)
        halo_back = lax.ppermute(back, 'cp', to_prev)
        return grad_u, tail, halo_back, g_wa, g_wi, vecs

    def full_fn(*args):
        lam_param = args[-1]
        grad_u, tail, halo_back, g_wa, g_wi, vecs = local_fn(*args)
        tail = jnp.swapaxes((tail + halo_back).astype(jnp.bfloat16), 0, 1)
        grad_u = lax.dynamic_update_slice(grad_u, tail, (0, grad_u.shape[1] - HALO, 0))
        g_wa, g_wi, vecs = lax.psum((g_wa, g_wi, vecs), 'cp')
        vecs = jnp.swapaxes(vecs, 0, 1).reshape(N_VEC, -1)
        g_lam = 8.0 * jax.nn.sigmoid(-lam_param) * vecs[GLAM]
        return (grad_u, vecs[GW:GW + CONV], vecs[GBC], g_wa, vecs[GBA], g_wi, vecs[GBI], g_lam)

    return jax.shard_map(full_fn, mesh=mesh,
                         in_specs=(seq_spec, P(None, 'cp'), seq_spec, rep_spec, rep_spec, rep_spec,
                                   rep_spec, rep_spec, rep_spec, rep_spec),
                         out_specs=(seq_spec,) + (rep_spec,) * 7, check_vma=False)
```

```python
import functools

import jax
import jax.numpy as jnp
from jax import lax
from jax.experimental import pallas as pl
from jax.experimental.pallas import tpu as pltpu
from jax.sharding import PartitionSpec as P

CONV = 4
HALO = CONV - 1
LOG2E = 1.4426950408889634
LANES = 128
STEPS = 8
LAG = 2
SLOTS = LAG + 1
ROWS = 8
PART_SLOTS, RECV_SLOTS, OWN_SLOTS, EDGE_SLOTS = 6, 4, 8, 4
STAGES = 8
MESH = pl.DeviceIdType.MESH

W0, BC, BA, BI, KL, KE = 0, 4, 5, 6, 7, 8
N_PAR = 16
GW, GBC, GBA, GBI, GLAM = 0, 4, 5, 6, 7
N_VEC = 8


def sigmoid_of(pre):
    root = lax.rsqrt(1.0 + jnp.exp2(pre * (-LOG2E)))
    return root * root


def decay_of(gate_r, par_kl, par_ke, keep):
    a_raw = jnp.exp2(gate_r * par_ke)
    gap = jnp.tanh(gate_r * (-par_kl)) * (1.0 + a_raw * a_raw)
    inv_root = lax.rsqrt(gap)
    decay = a_raw * keep
    mult = jnp.where(keep > 0.5, gap * inv_root, 1.0)
    return decay, mult, decay * decay * inv_root


def fold_rows(arr):
    return arr[:8] + arr[8:]


def dot_nn(lhs, rhs):
    return lax.dot_general(lhs, rhs, (((1,), (0,)), ((), ())), preferred_element_type=jnp.float32)


def dot_nt(lhs, rhs):
    return lax.dot_general(lhs, rhs, (((1,), (1,)), ((), ())), preferred_element_type=jnp.float32)


def dot_tn(lhs, rhs):
    return lax.dot_general(lhs, rhs, (((0,), (0,)), ((), ())), preferred_element_type=jnp.float32)


def fused_kernel(n_dev, n_heads,
                 u_ref, gh_ref, halo_ref, mask_ref, wa_ref, wi_ref, wa2_ref, wi2_ref, par_ref, par2_ref,
                 du_ref, grad_ref,
                 u_s, c_s, r_s, i_s, a_s, m_s, e_s, g_s, cb_s, h_scr, d_scr, ga_scr, gi_scr,
                 send, recv, resp, carry, part, got0, got1, got2, got3, own, vec_all, vec_ref, du_s, tail_s, edge_out, edge_in,
                 send_sem, recv_sem, give_sem, take_sem, sum_ssem, sum_rsem, edge_ssem, edge_rsem, du_sem, put_sem):
    n_batch, n_tok, width = u_ref.shape
    step_id = pl.program_id(0)
    me = lax.axis_index('cp')
    rows = 256
    span = rows // n_batch
    n_items = n_heads + 1
    core = lax.rem(me, 2)
    x_at = lax.rem(me // 2, 2)
    y_at = lax.rem(me // 4, 2)
    z_at = me // 8
    partner = me + 1 - 2 * core
    x_peer = me + 2 - 4 * x_at
    y_peer = me + 4 - 8 * y_at
    bit1 = x_at + core * (y_at - x_at)
    bit2 = y_at + core * (x_at - y_at)
    peer1 = x_peer + core * (y_peer - x_peer)
    peer2 = y_peer + core * (x_peer - y_peer)
    half_rows, quarter_rows = width // 2, width // 4
    piece = width // 16
    base1 = bit1 * half_rows
    base2 = base1 + bit2 * quarter_rows

    def row_range(start, count):
        return pl.ds(pl.multiple_of(start, count), count)

    def sum_copies(stage, item):
        p_at, r_at, o_at, s_at = (lax.rem(item, n) for n in (PART_SLOTS, RECV_SLOTS, OWN_SLOTS, OWN_SLOTS))

        def one(index, src, dst, dev):
            return pltpu.make_async_remote_copy(src_ref=src, dst_ref=dst, send_sem=sum_ssem.at[index, s_at],
                                                recv_sem=sum_rsem.at[index, s_at], device_id=(dev,), device_id_type=MESH)

        def z_peer(k):
            z_to = lax.rem(z_at + k, 4)
            return z_to, z_to * 8 + lax.rem(me, 8)

        if stage == 0:
            return [one(0, part.at[p_at, 1 - core], got0.at[r_at], partner)]
        if stage == 1:
            return [one(1, part.at[p_at, core, row_range((1 - bit1) * half_rows, half_rows)], got1.at[r_at], peer1)]
        if stage == 2:
            return [one(2, part.at[p_at, core, row_range(base1 + (1 - bit2) * quarter_rows, quarter_rows)], got2.at[r_at], peer2)]
        if stage == 3:
            return [one(2 + k, part.at[p_at, core, row_range(base2 + z_peer(k)[0] * piece, piece)], got3.at[r_at, k - 1], z_peer(k)[1])
                    for k in (1, 2, 3)]
        if stage == 4:
            mine = own.at[o_at, row_range(base2 + z_at * piece, piece)]
            return [one(5 + k, mine, mine, z_peer(k)[1]) for k in (1, 2, 3)]
        if stage == 5:
            mine = own.at[o_at, row_range(base2, quarter_rows)]
            return [one(9, mine, mine, peer2)]
        if stage == 6:
            mine = own.at[o_at, row_range(base1, half_rows)]
            return [one(10, mine, mine, peer1)]
        return [one(11, own.at[o_at], grad_ref.at[core, item], partner)]

    def put_copy(item):
        slot = lax.rem(item, OWN_SLOTS)
        return pltpu.make_async_copy(own.at[slot], grad_ref.at[core, item], put_sem.at[slot])

    def sum_stage(stage, item):
        p_at, r_at, o_at = (lax.rem(item, n) for n in (PART_SLOTS, RECV_SLOTS, OWN_SLOTS))
        for copy in sum_copies(stage - 1, item):
            copy.wait_recv()
            copy.wait_send()
        if stage == 1:
            part[p_at, core] = part[p_at, core] + got0[r_at]
        if stage == 2:
            at = row_range(base1, half_rows)
            part[p_at, core, at] = part[p_at, core, at] + got1[r_at]
        if stage == 3:
            at = row_range(base2, quarter_rows)
            part[p_at, core, at] = part[p_at, core, at] + got2[r_at]
        if stage == 4:
            at = row_range(base2 + z_at * piece, piece)
            own[o_at, at] = (part[p_at, core, at] + got3[r_at, 0]) + (got3[r_at, 1] + got3[r_at, 2])
        if stage == STAGES:
            put_copy(item).wait()
        else:
            for copy in sum_copies(stage, item):
                copy.start()
        if stage == STAGES - 1:
            put_copy(item).start()

    def edge_copy(head):
        slot = lax.rem(head, EDGE_SLOTS)
        return pltpu.make_async_remote_copy(src_ref=edge_out.at[slot], dst_ref=edge_in.at[slot], send_sem=edge_ssem.at[slot],
                                            recv_sem=edge_rsem.at[slot], device_id=(lax.rem(me + n_dev - 1, n_dev),), device_id_type=MESH)

    def du_copy(head):
        slot = lax.rem(head, EDGE_SLOTS)
        return pltpu.make_async_copy(du_s.at[slot], du_ref.at[:, :, pl.ds(pl.multiple_of(head * width, width), width)], du_sem.at[slot])

    def spread(src, dst, out_sem, in_sem, head, count):
        def one(k, _):
            dev = lax.rem(me + k, n_dev)
            pltpu.make_async_remote_copy(
                src_ref=src.at[head, pl.ds(pl.multiple_of(dev * ROWS, ROWS), count)],
                dst_ref=dst.at[head, pl.ds(pl.multiple_of(me * ROWS, ROWS), count)],
                send_sem=out_sem.at[head], recv_sem=in_sem.at[head],
                device_id=(dev,), device_id_type=pl.DeviceIdType.MESH).start()
            return 0
        lax.fori_loop(1, n_dev, one, 0)
        own = pl.ds(pl.multiple_of(me * ROWS, ROWS), ROWS)
        dst[head, own, :] = src[head, own, :]

    def settle(buf, sem, head, count):
        total = buf.at[head, pl.ds(0, (n_dev - 1) * count)]
        pltpu.make_async_copy(total, total, sem.at[head]).wait()

    @pl.when((step_id >= 1) & (step_id <= n_heads))
    def _combine():
        head = step_id - 1
        settle(recv, recv_sem, head, 3)
        state = jnp.zeros((1, LANES), jnp.float32)
        adj = jnp.zeros((1, LANES), jnp.float32)
        for dev in range(n_dev):
            row, back_row = dev * ROWS, (n_dev - 1 - dev) * ROWS
            resp[head, row:row + 1, :] = state
            resp[head, back_row + 1:back_row + 2, :] = adj
            state = recv[head, row:row + 1, :] * state + recv[head, row + 1:row + 2, :]
            adj = recv[head, back_row:back_row + 1, :] * adj + recv[head, back_row + 2:back_row + 3, :]
        spread(resp, carry, give_sem, take_sem, head, 2)

    @pl.when(step_id < n_heads)
    def _first():
        head = step_id
        slot = lax.rem(step_id, SLOTS)
        u_s[slot, :HALO] = halo_ref[...]
        for start in range(0, n_tok, 16):
            u_s[slot, HALO + start:HALO + start + 16] = jnp.swapaxes(u_ref[:, start:start + 16, :].astype(jnp.float32), 0, 1)
        for start in range(0, n_tok, 8):
            g_s[slot, start:start + 8] = jnp.swapaxes(gh_ref[:, start:start + 8, :], 0, 1)

        def conv_body(chunk, _):
            base = chunk * STEPS
            for step in range(STEPS):
                tok = base + step
                for lane in range(0, width, LANES):
                    cols = slice(lane, lane + LANES)
                    acc = par_ref[BC:BC + 1, cols] + par_ref[W0:W0 + 1, cols] * u_s[slot, tok + HALO, :, cols]
                    for tap in range(1, CONV):
                        acc = acc + par_ref[W0 + tap:W0 + tap + 1, cols] * (mask_ref[tap - 1, tok] * u_s[slot, tok + HALO - tap, :, cols])
                    c_s[slot, tok, :, cols] = acc
                    cb_s[slot, tok, :, cols] = acc.astype(jnp.bfloat16)
            return 0

        lax.fori_loop(0, n_tok // STEPS, conv_body, 0)
        for start in range(0, n_tok, span):
            part = cb_s[slot, start:start + span].reshape(rows, width)
            r_s[slot, start:start + span] = dot_nn(part, wa_ref[0]).reshape(span, n_batch, width)
            i_s[slot, start:start + span] = dot_nn(part, wi_ref[0]).reshape(span, n_batch, width)

        for half in range(width // LANES):
            cols = slice(half * LANES, (half + 1) * LANES)

            def fwd_body(chunk, run):
                state, prod = run
                base = chunk * STEPS
                for step in range(STEPS):
                    tok = base + step
                    gate_r = sigmoid_of(r_s[slot, tok, :, cols] + par_ref[BA:BA + 1, cols])
                    gate_i = sigmoid_of(i_s[slot, tok, :, cols] + par_ref[BI:BI + 1, cols])
                    decay, mult, ratio = decay_of(gate_r, par_ref[KL:KL + 1, cols], par_ref[KE:KE + 1, cols], mask_ref[0, tok])
                    r_s[slot, tok, :, cols] = gate_r
                    i_s[slot, tok, :, cols] = gate_i
                    a_s[slot, tok, :, cols] = decay
                    m_s[slot, tok, :, cols] = mult
                    e_s[slot, tok, :, cols] = ratio
                    state = decay * state + mult * (gate_i * c_s[slot, tok, :, cols])
                    prod = decay * prod
                return state, prod

            zero = jnp.zeros((n_batch, LANES), jnp.float32)
            state, prod = lax.fori_loop(0, n_tok // STEPS, fwd_body, (zero, zero + 1.0))

            def adj_body(chunk, adj):
                base = n_tok - STEPS - chunk * STEPS
                for step in reversed(range(STEPS)):
                    tok = base + step
                    adj = a_s[slot, tok, :, cols] * (g_s[slot, tok, :, cols] + adj)
                return adj

            first = lax.fori_loop(0, n_tok // STEPS, adj_body, zero)
            for row, val in enumerate((prod, state, first)):
                send.at[head][pl.ds(half * ROWS + row, n_batch, stride=2 * ROWS), :] = val
        spread(send, recv, send_sem, recv_sem, head, 3)

    for stage in reversed(range(1, STAGES + 1)):
        item_of = step_id - LAG - stage

        @pl.when((item_of >= 0) & (item_of < n_items))
        def _sum(stage=stage, item_of=item_of):
            sum_stage(stage, item_of)

    head_done = step_id - LAG - 2

    @pl.when((head_done >= 0) & (head_done < n_heads))
    def _stored():
        du_copy(head_done).wait()

    head_edge = step_id - LAG - 1

    @pl.when((head_edge >= 0) & (head_edge < n_heads))
    def _edge():
        slot = lax.rem(head_edge, EDGE_SLOTS)
        edge_copy(head_edge).wait_recv()
        edge_copy(head_edge).wait_send()
        du_s[slot, n_tok - HALO:] = (tail_s[slot] + edge_in[slot]).astype(jnp.bfloat16)
        du_copy(head_edge).start()

    @pl.when((step_id >= LAG) & (step_id < n_heads + LAG))
    def _second():
        head = step_id - LAG
        slot = lax.rem(step_id - LAG, SLOTS)
        e_at = lax.rem(head, EDGE_SLOTS)
        settle(carry, take_sem, head, 2)

        for half in range(width // LANES):
            cols = slice(half * LANES, (half + 1) * LANES)
            zero8 = jnp.zeros((8, LANES), jnp.float32)

            def fwd_body(chunk, state):
                base = chunk * STEPS
                for step in range(STEPS):
                    tok = base + step
                    h_scr[tok, :, cols] = state
                    state = a_s[slot, tok, :, cols] * state + m_s[slot, tok, :, cols] * (i_s[slot, tok, :, cols] * c_s[slot, tok, :, cols])
                return state

            lax.fori_loop(0, n_tok // STEPS, fwd_body, carry.at[head][pl.ds(half * ROWS, n_batch, stride=2 * ROWS), :])

            def bwd_body(chunk, run):
                adj_next, sum_a, sum_i, sum_l = run
                base = n_tok - STEPS - chunk * STEPS
                for step in reversed(range(STEPS)):
                    tok = base + step
                    gate_r = r_s[slot, tok, :, cols]
                    gate_i = i_s[slot, tok, :, cols]
                    conv_c = c_s[slot, tok, :, cols]
                    adj = g_s[slot, tok, :, cols] + adj_next
                    adj_next = a_s[slot, tok, :, cols] * adj
                    d_log = adj_next * h_scr[tok, :, cols] - adj * (gate_i * conv_c) * e_s[slot, tok, :, cols]
                    direct = adj * m_s[slot, tok, :, cols] * gate_i
                    d_pre_i = direct * conv_c * (1.0 - gate_i)
                    d_log_r = d_log * gate_r
                    d_pre_a = d_log_r * (par2_ref[KL:KL + 1, cols] * (1.0 - gate_r))
                    sum_l = sum_l + fold_rows(d_log_r)
                    sum_a = sum_a + fold_rows(d_pre_a)
                    sum_i = sum_i + fold_rows(d_pre_i)
                    d_scr[tok, :, cols] = direct
                    ga_scr[tok, :, cols] = d_pre_a.astype(jnp.bfloat16)
                    gi_scr[tok, :, cols] = d_pre_i.astype(jnp.bfloat16)
                return adj_next, sum_a, sum_i, sum_l

            adj_in = carry.at[head][pl.ds(half * ROWS + 1, n_batch, stride=2 * ROWS), :]
            _, sum_a, sum_i, sum_l = lax.fori_loop(0, n_tok // STEPS, bwd_body, (adj_in, zero8, zero8, zero8))
            vec_ref[GBA:GBA + 1, cols] = jnp.sum(sum_a, axis=0, keepdims=True)
            vec_ref[GBI:GBI + 1, cols] = jnp.sum(sum_i, axis=0, keepdims=True)
            vec_ref[GLAM:GLAM + 1, cols] = jnp.sum(sum_l, axis=0, keepdims=True)

        for start in range(0, n_tok, span):
            toks = slice(start, start + span)
            back = dot_nt(ga_scr[toks].reshape(rows, width), wa2_ref[0]) + dot_nt(gi_scr[toks].reshape(rows, width), wi2_ref[0])
            d_scr[toks] = d_scr[toks] + back.reshape(span, n_batch, width)
        all_c = cb_s[slot].reshape(n_tok * n_batch, width)
        p_at = lax.rem(head, PART_SLOTS)
        part[p_at, 0] = dot_tn(all_c, ga_scr[...].reshape(n_tok * n_batch, width))
        part[p_at, 1] = dot_tn(all_c, gi_scr[...].reshape(n_tok * n_batch, width))

        for half in range(width // LANES):
            cols = slice(half * LANES, (half + 1) * LANES)
            zero8 = jnp.zeros((8, LANES), jnp.float32)
            zero = jnp.zeros((n_batch, LANES), jnp.float32)

            def tap_body(chunk, run):
                sums = list(run[:CONV + 1])
                ahead = list(run[CONV + 1:])
                last = [None] * HALO
                base = n_tok - STEPS - chunk * STEPS
                for step in reversed(range(STEPS)):
                    tok = base + step
                    d_conv = d_scr[tok, :, cols]
                    sums[CONV] = sums[CONV] + fold_rows(d_conv)
                    masked = [d_conv] + [mask_ref[tap - 1, tok] * d_conv for tap in range(1, CONV)]
                    for tap in range(CONV):
                        sums[tap] = sums[tap] + fold_rows(masked[tap] * u_s[slot, tok + HALO - tap, :, cols])
                    terms = [par2_ref[W0 + tap:W0 + tap + 1, cols] * masked[tap] for tap in range(CONV)]
                    d_u = ahead[0] + terms[0]
                    du_s[e_at, tok, :, cols] = d_u.astype(jnp.bfloat16)
                    if step >= STEPS - HALO:
                        last[step - STEPS + HALO] = d_u
                    ahead = [ahead[1] + terms[1], ahead[2] + terms[2], terms[3]]
                return tuple(sums) + tuple(ahead) + tuple(last)

            def tap_loop(first, stop, run):
                return lax.fori_loop(first, stop, lambda chunk, val: tap_body(chunk, val)[:-HALO], run)

            begin = tap_body(0, (zero8,) * (CONV + 1) + (zero,) * HALO)
            for row in range(HALO):
                tail_s[e_at, row, :, cols] = begin[-HALO + row]
            out = tap_loop(1, n_tok // STEPS, begin[:-HALO])
            for row in range(CONV + 1):
                vec_ref[GW + row:GW + row + 1, cols] = jnp.sum(out[row], axis=0, keepdims=True)
            for row in range(HALO):
                edge_out[e_at, HALO - 1 - row, :, cols] = out[CONV + 1 + row]
        edge_copy(head).start()
        vec_all[pl.ds(pl.multiple_of(head * N_VEC, N_VEC), N_VEC), :] = vec_ref[...]

    @pl.when(step_id == 0)
    def _clear():
        vec_all[...] = jnp.zeros_like(vec_all)

    item_new = step_id - LAG

    @pl.when(item_new == n_heads)
    def _pack():
        p_at = lax.rem(item_new, PART_SLOTS)
        part[p_at, 0] = vec_all[...]
        part[p_at, 1] = jnp.zeros_like(vec_all)

    @pl.when((item_new >= 0) & (item_new < n_items))
    def _share():
        for copy in sum_copies(0, item_new):
            copy.start()

    @pl.when(step_id == n_heads - 1 + LAG)
    def _drain():
        def one(head, _):
            settle(send, send_sem, head, 3)
            settle(resp, give_sem, head, 2)
            return 0
        lax.fori_loop(0, n_heads, one, 0)


def solution(mesh):
    n_dev = mesh.shape['cp']
    to_next = [(src, src + 1) for src in range(n_dev - 1)]
    seq_spec = P(None, 'cp', None)
    rep_spec = P()

    def local_fn(u_in, seg_ids, grad_h, conv_w, conv_b, a_gate_w, a_gate_b, x_gate_w, x_gate_b, lam_param):
        n_batch, n_tok, n_width = u_in.shape
        n_heads, block_w, _ = a_gate_w.shape
        has_prev = lax.axis_index('cp') > 0
        tail_pack = jnp.concatenate([u_in[:, n_tok - HALO:, :].astype(jnp.float32),
                                     seg_ids[:, n_tok - HALO:, None].astype(jnp.float32)], axis=2)
        recv_pack = lax.ppermute(tail_pack, 'cp', to_next)
        halo_u = jnp.swapaxes(recv_pack[:, :, :n_width], 0, 1)
        halo_seg = recv_pack[:, :, n_width].astype(jnp.int32)
        seg_ext = jnp.concatenate([halo_seg, seg_ids], axis=1).T
        ext_ok = (jnp.arange(n_tok + HALO) >= HALO) | has_prev
        masks = []
        for tap in range(1, CONV):
            tap_ok = (seg_ext[HALO - tap:HALO - tap + n_tok] == seg_ext[HALO:]) & ext_ok[HALO - tap:HALO - tap + n_tok, None]
            masks.append(tap_ok.astype(jnp.float32))
        masks = jnp.broadcast_to(jnp.stack(masks)[..., None], (HALO, n_tok, n_batch, LANES))
        log_rate = -8.0 * jax.nn.softplus(-lam_param)
        par = jnp.concatenate([conv_w, conv_b[None], a_gate_b[None], x_gate_b[None], log_rate[None], log_rate[None] * LOG2E,
                               jnp.zeros((N_PAR - 9, n_width), jnp.float32)], axis=0)

        def now(step):
            return jnp.minimum(step, n_heads - 1)

        def late(step):
            return jnp.clip(step - LAG, 0, n_heads - 1)

        def blk_row(at):
            return pl.BlockSpec((n_batch, n_tok, block_w), lambda s: (0, 0, at(s)))

        def blk_time(count, at):
            return pl.BlockSpec((count, n_batch, block_w), lambda s: (0, 0, at(s)))

        def mat_spec(at):
            return pl.BlockSpec((1, block_w, block_w), lambda s: (at(s), 0, 0))

        def par_spec(at):
            return pl.BlockSpec((N_PAR, block_w), lambda s: (0, at(s)))

        mask_spec = pl.BlockSpec((HALO, n_tok, n_batch, LANES), lambda s: (0, 0, 0, 0))
        f32_slots = pltpu.VMEM((SLOTS, n_tok, n_batch, block_w), jnp.float32)
        f32_scr = pltpu.VMEM((n_tok, n_batch, block_w), jnp.float32)
        bf_scr = pltpu.VMEM((n_tok, n_batch, block_w), jnp.bfloat16)
        wire = pltpu.VMEM((n_heads, n_dev * ROWS, LANES), jnp.float32)
        sems = pltpu.SemaphoreType.DMA((n_heads,))

        item_f32 = functools.partial(pltpu.VMEM, dtype=jnp.float32)
        n_sems = 12
        du_time, grads = pl.pallas_call(
            functools.partial(fused_kernel, n_dev, n_heads), grid=(n_heads + 1 + LAG + STAGES,),
            in_specs=[blk_row(now), blk_row(now), blk_time(HALO, now), mask_spec, mat_spec(now), mat_spec(now),
                      mat_spec(late), mat_spec(late), par_spec(now), par_spec(late)],
            out_specs=[pl.BlockSpec(memory_space=pl.ANY)] * 2,
            out_shape=[jax.ShapeDtypeStruct((n_tok, n_batch, n_width), jnp.bfloat16),
                       jax.ShapeDtypeStruct((2, n_heads + 1, block_w, block_w), jnp.float32)],
            scratch_shapes=[pltpu.VMEM((SLOTS, n_tok + HALO, n_batch, block_w), jnp.float32)] + [f32_slots] * 7
            + [pltpu.VMEM((SLOTS, n_tok, n_batch, block_w), jnp.bfloat16), f32_scr, f32_scr, bf_scr, bf_scr] + [wire] * 4
            + [item_f32((PART_SLOTS, 2, block_w, block_w)), item_f32((RECV_SLOTS, block_w, block_w)),
               item_f32((RECV_SLOTS, block_w // 2, block_w)), item_f32((RECV_SLOTS, block_w // 4, block_w)),
               item_f32((RECV_SLOTS, 3, block_w // 16, block_w)), item_f32((OWN_SLOTS, block_w, block_w)),
               item_f32((block_w, block_w)), item_f32((N_VEC, block_w)),
               pltpu.VMEM((EDGE_SLOTS, n_tok, n_batch, block_w), jnp.bfloat16)]
            + [item_f32((EDGE_SLOTS, HALO, n_batch, block_w))] * 3
            + [sems] * 4 + [pltpu.SemaphoreType.DMA((n_sems, OWN_SLOTS))] * 2
            + [pltpu.SemaphoreType.DMA((EDGE_SLOTS,))] * 3 + [pltpu.SemaphoreType.DMA((OWN_SLOTS,))],
            compiler_params=pltpu.CompilerParams(vmem_limit_bytes=67043328, has_side_effects=True), name='fused_pass',
        )(u_in, grad_h, halo_u, masks, a_gate_w, x_gate_w, a_gate_w, x_gate_w, par, par)
        vecs = grads[0, n_heads, :n_heads * N_VEC].reshape(n_heads, N_VEC, block_w)
        vecs = jnp.swapaxes(vecs, 0, 1).reshape(N_VEC, n_width)
        g_lam = 8.0 * jax.nn.sigmoid(-lam_param) * vecs[GLAM]
        return (jnp.swapaxes(du_time, 0, 1), vecs[GW:GW + CONV], vecs[GBC], grads[0, :n_heads], vecs[GBA],
                grads[1, :n_heads], vecs[GBI], g_lam)

    return jax.shard_map(local_fn, mesh=mesh,
                         in_specs=(seq_spec, P(None, 'cp'), seq_spec, rep_spec, rep_spec, rep_spec,
                                   rep_spec, rep_spec, rep_spec, rep_spec),
                         out_specs=(seq_spec,) + (rep_spec,) * 7, check_vma=False)
```

```python
import functools

import jax
import jax.numpy as jnp
from jax import lax
from jax.experimental import pallas as pl
from jax.experimental.pallas import tpu as pltpu
from jax.sharding import PartitionSpec as P

CONV = 4
HALO = CONV - 1
LOG2E = 1.4426950408889634
LN2 = 0.6931471805599453
START_BIAS = -1e4
LANES = 128
STEPS = 16
BLOCK = 16
LAG = 3
SLOTS = LAG + 1
GROUP, DEPTH = 8, 4
SUM_ROWS, IN_ROWS = 12, 8
PITCH = 16
PART_SLOTS, RECV_SLOTS, OWN_SLOTS, EDGE_SLOTS, EDGE_IN = 6, 4, 8, 4, 8
STAGES, FIRST_SLOTS = 8, 4
AFTER = (0, 1, 2, 3, 4, 5, 6, 7, 8)
MESH = pl.DeviceIdType.MESH

W0, BC, BA, BI, KL, KE = 0, 4, 5, 6, 7, 8
N_PAR = 16
GW, GBC, GBA, GBI, GLAM = 0, 4, 5, 6, 7
N_VEC = 8


def sigmoid_of(pre):
    root = lax.rsqrt(1.0 + jnp.exp2(pre * (-LOG2E)))
    return root * root


def decay_of(gate_r, par_ke, bias):
    log_two = gate_r * par_ke + bias
    decay = jnp.exp2(log_two)
    square = decay * decay
    gap = jnp.tanh(log_two * (-LN2)) * (1.0 + square)
    inv_root = lax.rsqrt(gap)
    return decay, gap * inv_root, square * inv_root * inv_root


def fold_rows(arr):
    return arr[:8] + arr[8:]


def dot_nn(lhs, rhs):
    return lax.dot_general(lhs, rhs, (((1,), (0,)), ((), ())), preferred_element_type=jnp.float32)


def dot_nt(lhs, rhs):
    return lax.dot_general(lhs, rhs, (((1,), (1,)), ((), ())), preferred_element_type=jnp.float32)


def dot_tn(lhs, rhs):
    return lax.dot_general(lhs, rhs, (((0,), (0,)), ((), ())), preferred_element_type=jnp.float32)


def fused_kernel(n_dev, n_heads,
                 u_ref, tail_ref, gh_ref, mask_ref, wa_ref, wi_ref, wa2_ref, wi2_ref, par_ref, par2_ref,
                 du_ref, grad_ref,
                 u_s, c_s, r_s, i_s, a_s, m_s, e_s, g_s, cb_s, h_scr, d_scr, ga_scr, gi_scr,
                 send, recv, group, resp, carry, halo_out, halo_in, part, got0, got1, got2, got3, own, vec_all, vec_ref, du_s, tail_s, edge_out, edge_in,
                 send_sem, recv_sem, group_ssem, group_rsem, give_sem, take_sem, halo_ssem, halo_rsem, sum_ssem, sum_rsem, edge_ssem, edge_rsem, du_sem, put_sem):
    n_batch, n_tok, width = u_ref.shape
    step_id = pl.program_id(0)
    me = lax.axis_index('cp')
    rows = 256
    core = lax.rem(me, 2)
    x_at = lax.rem(me // 2, 2)
    y_at = lax.rem(me // 4, 2)
    z_at = me // GROUP
    place = lax.rem(me, GROUP)
    partner = me + 1 - 2 * core
    x_peer = me + 2 - 4 * x_at
    y_peer = me + 4 - 8 * y_at
    bit1 = x_at + core * (y_at - x_at)
    bit2 = y_at + core * (x_at - y_at)
    peer1 = x_peer + core * (y_peer - x_peer)
    peer2 = y_peer + core * (x_peer - y_peer)
    half_rows, quarter_rows = width // 2, width // 4
    piece = width // 16
    base1 = bit1 * half_rows
    base2 = base1 + bit2 * quarter_rows

    def row_range(start, count):
        return pl.ds(pl.multiple_of(start, count), count)

    def sum_copies(stage, item):
        p_at, r_at, o_at, s_at, f_at = (lax.rem(item, n) for n in (PART_SLOTS, RECV_SLOTS, OWN_SLOTS, OWN_SLOTS, FIRST_SLOTS))

        def one(index, src, dst, dev):
            return pltpu.make_async_remote_copy(src_ref=src, dst_ref=dst, send_sem=sum_ssem.at[index, s_at],
                                                recv_sem=sum_rsem.at[index, s_at], device_id=(dev,), device_id_type=MESH)

        def z_peer(k):
            z_to = lax.rem(z_at + k, 4)
            return z_to, z_to * GROUP + place

        if stage == 0:
            return [one(0, part.at[p_at, 1 - core], got0.at[f_at], partner)]
        if stage == 1:
            return [one(1, part.at[p_at, core, row_range((1 - bit1) * half_rows, half_rows)], got1.at[r_at], peer1)]
        if stage == 2:
            return [one(2, part.at[p_at, core, row_range(base1 + (1 - bit2) * quarter_rows, quarter_rows)], got2.at[r_at], peer2)]
        if stage == 3:
            return [one(2 + k, part.at[p_at, core, row_range(base2 + z_peer(k)[0] * piece, piece)], got3.at[r_at, k - 1], z_peer(k)[1])
                    for k in (1, 2, 3)]
        if stage == 4:
            mine = own.at[o_at, row_range(base2 + z_at * piece, piece)]
            return [one(5 + k, mine, mine, z_peer(k)[1]) for k in (1, 2, 3)]
        if stage == 5:
            mine = own.at[o_at, row_range(base2, quarter_rows)]
            return [one(9, mine, mine, peer2)]
        if stage == 6:
            mine = own.at[o_at, row_range(base1, half_rows)]
            return [one(10, mine, mine, peer1)]
        return [one(11, own.at[o_at], grad_ref.at[core, item], partner)]

    def put_copy(item):
        slot = lax.rem(item, OWN_SLOTS)
        return pltpu.make_async_copy(own.at[slot], grad_ref.at[core, item], put_sem.at[slot])

    def sum_stage(stage, item):
        p_at, r_at, o_at = (lax.rem(item, n) for n in (PART_SLOTS, RECV_SLOTS, OWN_SLOTS))
        for copy in sum_copies(stage - 1, item):
            copy.wait_recv()
            copy.wait_send()
        if stage == 1:
            part[p_at, core] = part[p_at, core] + got0[lax.rem(item, FIRST_SLOTS)]
        if stage == 2:
            at = row_range(base1, half_rows)
            part[p_at, core, at] = part[p_at, core, at] + got1[r_at]
        if stage == 3:
            at = row_range(base2, quarter_rows)
            part[p_at, core, at] = part[p_at, core, at] + got2[r_at]
        if stage == 4:
            at = row_range(base2 + z_at * piece, piece)
            own[o_at, at] = (part[p_at, core, at] + got3[r_at, 0]) + (got3[r_at, 1] + got3[r_at, 2])
        if stage == STAGES:
            put_copy(item).wait()
        else:
            for copy in sum_copies(stage, item):
                copy.start()
        if stage == STAGES - 1:
            put_copy(item).start()

    def edge_copy(head):
        slot, to = lax.rem(head, EDGE_SLOTS), lax.rem(head, EDGE_IN)
        return pltpu.make_async_remote_copy(src_ref=edge_out.at[slot], dst_ref=edge_in.at[to], send_sem=edge_ssem.at[slot],
                                            recv_sem=edge_rsem.at[to], device_id=(lax.rem(me + n_dev - 1, n_dev),), device_id_type=MESH)

    def du_copy(head):
        slot = lax.rem(head, EDGE_SLOTS)
        return pltpu.make_async_copy(du_s.at[slot], du_ref.at[:, :, pl.ds(pl.multiple_of(head * width, width), width)], du_sem.at[slot])

    def block_of(index, pitch, count):
        return pl.ds(pl.multiple_of(index * pitch, pitch), count)

    def spread(src, dst, out_sem, in_sem, head, pitch, count):
        def one(k, _):
            to = lax.rem(place + k, GROUP)
            pltpu.make_async_remote_copy(
                src_ref=src.at[head, block_of(to, pitch, count)], dst_ref=dst.at[head, block_of(place, pitch, count)],
                send_sem=out_sem.at[head], recv_sem=in_sem.at[head],
                device_id=(z_at * GROUP + to,), device_id_type=MESH).start()
            return 0
        lax.fori_loop(1, GROUP, one, 0, unroll=True)
        own_rows = block_of(place, pitch, pitch)
        dst[head, own_rows, :] = src[head, own_rows, :]

    def settle(buf, sem, head, total):
        all_rows = buf.at[head, pl.ds(0, total)]
        pltpu.make_async_copy(all_rows, all_rows, sem.at[head]).wait()

    def rows_of(buf, head, index, quantity):
        start = index * PITCH + 4 * quantity
        return buf[head, start:start + 4, :]

    def halo_copy(head):
        slot = lax.rem(head, EDGE_SLOTS)
        return pltpu.make_async_remote_copy(src_ref=halo_out.at[slot], dst_ref=halo_in.at[slot], send_sem=halo_ssem.at[slot],
                                            recv_sem=halo_rsem.at[slot], device_id=(lax.rem(me + 1, n_dev),), device_id_type=MESH)

    def halo_send(head, src_ref):
        last = jnp.swapaxes(src_ref[:, src_ref.shape[1] - BLOCK:, :].astype(jnp.float32), 0, 1)
        halo_out[lax.rem(head, EDGE_SLOTS)] = last[BLOCK - HALO:]
        halo_copy(head).start()

    @pl.when(step_id == 0)
    def _begin():
        vec_all[...] = jnp.zeros_like(vec_all)
        halo_send(0, u_ref)

    def group_copies(head):
        mine = group.at[head, block_of(z_at, PITCH, SUM_ROWS)]
        return [pltpu.make_async_remote_copy(src_ref=mine, dst_ref=mine, send_sem=group_ssem.at[k, head], recv_sem=group_rsem.at[k, head],
                                             device_id=(lax.rem(z_at + 1 + k, DEPTH) * GROUP + place,), device_id_type=MESH)
                for k in range(DEPTH - 1)]

    def combine(head):
        for copy in group_copies(head):
            copy.wait_recv()
            copy.wait_send()
        state = jnp.zeros((4, LANES), jnp.float32)
        adj = jnp.zeros((4, LANES), jnp.float32)
        for index in range(DEPTH - 1):
            step_state = rows_of(group, head, index, 0) * state + rows_of(group, head, index, 1)
            state = jnp.where(index < z_at, step_state, state)
            other = DEPTH - 1 - index
            step_adj = rows_of(group, head, other, 0) * adj + rows_of(group, head, other, 2)
            adj = jnp.where(other > z_at, step_adj, adj)
        for index in range(GROUP):
            other = GROUP - 1 - index
            resp[head, index * IN_ROWS:index * IN_ROWS + 4, :] = state
            resp[head, other * IN_ROWS + 4:other * IN_ROWS + 8, :] = adj
            state = rows_of(recv, head, index, 0) * state + rows_of(recv, head, index, 1)
            adj = rows_of(recv, head, other, 0) * adj + rows_of(recv, head, other, 2)
        spread(resp, carry, give_sem, take_sem, head, IN_ROWS, IN_ROWS)

    def put_rows(head, quantity, half, val):
        for high in range(2):
            send.at[head][pl.ds(4 * quantity + 2 * high + half, GROUP, stride=PITCH), :] = val[high * GROUP:(high + 1) * GROUP]

    def take_rows(head, quantity, half):
        return jnp.concatenate([carry.at[head][pl.ds(4 * quantity + 2 * high + half, GROUP, stride=IN_ROWS), :] for high in range(2)], axis=0)

    @pl.when(step_id < n_heads)
    def _first():
        head = step_id
        slot = lax.rem(step_id, SLOTS)
        halo_copy(head).wait_recv()
        halo_copy(head).wait_send()
        u_s[slot, :HALO] = halo_in[lax.rem(head, EDGE_SLOTS)]

        @pl.when(head + 1 < n_heads)
        def _next_halo():
            halo_send(head + 1, tail_ref)

        for start in range(0, n_tok, BLOCK):
            u_s[slot, HALO + start:HALO + start + BLOCK] = jnp.swapaxes(u_ref[:, start:start + BLOCK, :].astype(jnp.float32), 0, 1)
            for tok in range(start, start + BLOCK):
                for lane in range(0, width, LANES):
                    cols = slice(lane, lane + LANES)
                    acc = par_ref[BC:BC + 1, cols] + par_ref[W0:W0 + 1, cols] * u_s[slot, tok + HALO, :, cols]
                    for tap in range(1, CONV):
                        acc = acc + par_ref[W0 + tap:W0 + tap + 1, cols] * (mask_ref[tap - 1, tok] * u_s[slot, tok + HALO - tap, :, cols])
                    c_s[slot, tok, :, cols] = acc
                    cb_s[slot, tok, :, cols] = acc.astype(jnp.bfloat16)
            g_s[slot, start:start + BLOCK] = jnp.swapaxes(gh_ref[:, start:start + BLOCK, :], 0, 1)
            part_c = cb_s[slot, start:start + BLOCK].reshape(rows, width)
            r_s[slot, start:start + BLOCK] = dot_nn(part_c, wa_ref[0]).reshape(BLOCK, n_batch, width)
            i_s[slot, start:start + BLOCK] = dot_nn(part_c, wi_ref[0]).reshape(BLOCK, n_batch, width)

        for half in range(width // LANES):
            cols = slice(half * LANES, (half + 1) * LANES)

            def fwd_body(chunk, run):
                state, prod = run
                base = chunk * STEPS
                for step in range(STEPS):
                    tok = base + step
                    gate_r = sigmoid_of(r_s[slot, tok, :, cols] + par_ref[BA:BA + 1, cols])
                    gate_i = sigmoid_of(i_s[slot, tok, :, cols] + par_ref[BI:BI + 1, cols])
                    decay, mult, ratio = decay_of(gate_r, par_ref[KE:KE + 1, cols], mask_ref[HALO, tok])
                    r_s[slot, tok, :, cols] = gate_r
                    i_s[slot, tok, :, cols] = gate_i
                    a_s[slot, tok, :, cols] = decay
                    m_s[slot, tok, :, cols] = mult
                    e_s[slot, tok, :, cols] = ratio
                    state = decay * state + mult * (gate_i * c_s[slot, tok, :, cols])
                    prod = decay * prod
                return state, prod

            zero = jnp.zeros((n_batch, LANES), jnp.float32)
            state, prod = lax.fori_loop(0, n_tok // STEPS, fwd_body, (zero, zero + 1.0))

            put_rows(head, 0, half, prod)
            put_rows(head, 1, half, state)

        def adj_body(chunk, adj):
            base = n_tok - STEPS - chunk * STEPS
            for step in reversed(range(STEPS)):
                tok = base + step
                adj = a_s[slot, tok] * (g_s[slot, tok] + adj)
            return adj

        first = lax.fori_loop(0, n_tok // STEPS, adj_body, jnp.zeros((n_batch, width), jnp.float32))
        for half in range(width // LANES):
            put_rows(head, 2, half, first[:, half * LANES:(half + 1) * LANES])
        spread(send, recv, send_sem, recv_sem, head, PITCH, SUM_ROWS)

    @pl.when((step_id >= 2) & (step_id <= n_heads + 1))
    def _combine():
        combine(step_id - 2)

    @pl.when((step_id >= 1) & (step_id <= n_heads))
    def _group():
        head = step_id - 1
        settle(recv, recv_sem, head, (GROUP - 1) * SUM_ROWS)
        prod = jnp.ones((4, LANES), jnp.float32)
        state = jnp.zeros((4, LANES), jnp.float32)
        adj = jnp.zeros((4, LANES), jnp.float32)
        for index in range(GROUP):
            decay = rows_of(recv, head, index, 0)
            state = decay * state + rows_of(recv, head, index, 1)
            prod = decay * prod
            other = GROUP - 1 - index
            adj = rows_of(recv, head, other, 0) * adj + rows_of(recv, head, other, 2)
        mine = block_of(z_at, PITCH, PITCH)
        group[head, mine, :] = jnp.concatenate([prod, state, adj, jnp.zeros_like(adj)], axis=0)
        for copy in group_copies(head):
            copy.start()

    for stage in reversed(range(1, STAGES + 1)):
        item_of = step_id - LAG - AFTER[stage]

        @pl.when((item_of >= 0) & (item_of < n_heads))
        def _sum(stage=stage, item_of=item_of):
            sum_stage(stage, item_of)

        @pl.when(item_of == n_heads - 1)
        def _sum_vectors(stage=stage):
            sum_stage(stage, n_heads)

    head_done = step_id - LAG - 3

    @pl.when((head_done >= 0) & (head_done < n_heads))
    def _stored():
        du_copy(head_done).wait()

    head_edge = step_id - LAG - 2

    @pl.when((head_edge >= 0) & (head_edge < n_heads))
    def _edge():
        slot = lax.rem(head_edge, EDGE_SLOTS)
        edge_copy(head_edge).wait_recv()
        edge_copy(head_edge).wait_send()
        du_s[slot, n_tok - HALO:] = (tail_s[slot] + edge_in[lax.rem(head_edge, EDGE_IN)]).astype(jnp.bfloat16)
        du_copy(head_edge).start()

    @pl.when((step_id >= LAG) & (step_id < n_heads + LAG))
    def _second():
        head = step_id - LAG
        slot = lax.rem(step_id - LAG, SLOTS)
        e_at = lax.rem(head, EDGE_SLOTS)
        settle(carry, take_sem, head, (GROUP - 1) * IN_ROWS)

        def state_body(chunk, state):
            base = chunk * STEPS
            for step in range(STEPS):
                tok = base + step
                h_scr[tok] = state
                state = a_s[slot, tok] * state + m_s[slot, tok] * (i_s[slot, tok] * c_s[slot, tok])
            return state

        state_in = [take_rows(head, 0, half) for half in range(width // LANES)]
        lax.fori_loop(0, n_tok // STEPS, state_body, jnp.concatenate(state_in, axis=1))

        for half in range(width // LANES):
            cols = slice(half * LANES, (half + 1) * LANES)
            zero8 = jnp.zeros((8, LANES), jnp.float32)

            def bwd_body(chunk, run):
                adj_next, sum_a, sum_i, sum_l = run
                base = n_tok - STEPS - chunk * STEPS
                for step in reversed(range(STEPS)):
                    tok = base + step
                    gate_r = r_s[slot, tok, :, cols]
                    gate_i = i_s[slot, tok, :, cols]
                    conv_c = c_s[slot, tok, :, cols]
                    adj = g_s[slot, tok, :, cols] + adj_next
                    adj_next = a_s[slot, tok, :, cols] * adj
                    direct = adj * m_s[slot, tok, :, cols] * gate_i
                    d_input = direct * conv_c
                    d_pre_i = d_input * (1.0 - gate_i)
                    d_log = adj_next * h_scr[tok, :, cols] - d_input * e_s[slot, tok, :, cols]
                    d_log_r = d_log * gate_r
                    d_pre_a = d_log_r * (par2_ref[KL:KL + 1, cols] * (1.0 - gate_r))
                    sum_l = sum_l + fold_rows(d_log_r)
                    sum_a = sum_a + fold_rows(d_pre_a)
                    sum_i = sum_i + fold_rows(d_pre_i)
                    d_scr[tok, :, cols] = direct
                    ga_scr[tok, :, cols] = d_pre_a.astype(jnp.bfloat16)
                    gi_scr[tok, :, cols] = d_pre_i.astype(jnp.bfloat16)
                return adj_next, sum_a, sum_i, sum_l

            adj_in = take_rows(head, 1, half)
            _, sum_a, sum_i, sum_l = lax.fori_loop(0, n_tok // STEPS, bwd_body, (adj_in, zero8, zero8, zero8))
            vec_ref[GBA:GBA + 1, cols] = jnp.sum(sum_a, axis=0, keepdims=True)
            vec_ref[GBI:GBI + 1, cols] = jnp.sum(sum_i, axis=0, keepdims=True)
            vec_ref[GLAM:GLAM + 1, cols] = jnp.sum(sum_l, axis=0, keepdims=True)

        p_at = lax.rem(head, PART_SLOTS)
        all_c = cb_s[slot].reshape(n_tok * n_batch, width)
        part[p_at, 0] = dot_tn(all_c, ga_scr[...].reshape(n_tok * n_batch, width))
        part[p_at, 1] = dot_tn(all_c, gi_scr[...].reshape(n_tok * n_batch, width))

        halves = width // LANES
        sums = [[jnp.zeros((8, LANES), jnp.float32)] * (CONV + 1) for _ in range(halves)]
        ahead = [[jnp.zeros((n_batch, LANES), jnp.float32)] * HALO for _ in range(halves)]
        for start in reversed(range(0, n_tok, BLOCK)):
            toks = slice(start, start + BLOCK)
            back = dot_nt(ga_scr[toks].reshape(rows, width), wa2_ref[0]) + dot_nt(gi_scr[toks].reshape(rows, width), wi2_ref[0])
            d_scr[toks] = d_scr[toks] + back.reshape(BLOCK, n_batch, width)
            for half in range(halves):
                cols = slice(half * LANES, (half + 1) * LANES)
                tot, nxt = sums[half], ahead[half]
                for tok in reversed(range(start, start + BLOCK)):
                    d_conv = d_scr[tok, :, cols]
                    tot[CONV] = tot[CONV] + fold_rows(d_conv)
                    masked = [d_conv] + [mask_ref[tap - 1, tok] * d_conv for tap in range(1, CONV)]
                    for tap in range(CONV):
                        tot[tap] = tot[tap] + fold_rows(masked[tap] * u_s[slot, tok + HALO - tap, :, cols])
                    terms = [par2_ref[W0 + tap:W0 + tap + 1, cols] * masked[tap] for tap in range(CONV)]
                    d_u = nxt[0] + terms[0]
                    du_s[e_at, tok, :, cols] = d_u.astype(jnp.bfloat16)
                    if tok >= n_tok - HALO:
                        tail_s[e_at, tok - n_tok + HALO, :, cols] = d_u
                    nxt = [nxt[1] + terms[1], nxt[2] + terms[2], terms[3]]
                ahead[half] = nxt
        for half in range(halves):
            cols = slice(half * LANES, (half + 1) * LANES)
            for row in range(CONV + 1):
                vec_ref[GW + row:GW + row + 1, cols] = jnp.sum(sums[half][row], axis=0, keepdims=True)
            for row in range(HALO):
                edge_out[e_at, HALO - 1 - row, :, cols] = ahead[half][row]
        edge_copy(head).start()
        vec_all[pl.ds(pl.multiple_of(head * N_VEC, N_VEC), N_VEC), :] = vec_ref[...]

    item_new = step_id - LAG

    @pl.when((item_new >= 0) & (item_new < n_heads))
    def _share():
        for copy in sum_copies(0, item_new):
            copy.start()

    @pl.when(item_new == n_heads - 1)
    def _share_vectors():
        p_at = n_heads % PART_SLOTS
        part[p_at, 0] = vec_all[...]
        part[p_at, 1] = jnp.zeros_like(vec_all)
        for copy in sum_copies(0, n_heads):
            copy.start()

    @pl.when(step_id == n_heads - 1 + LAG)
    def _drain():
        def one(head, _):
            settle(send, send_sem, head, (GROUP - 1) * SUM_ROWS)
            settle(resp, give_sem, head, (GROUP - 1) * IN_ROWS)
            return 0
        lax.fori_loop(0, n_heads, one, 0)


def solution(mesh):
    n_dev = mesh.shape['cp']
    to_next = [(src, src + 1) for src in range(n_dev - 1)]
    seq_spec = P(None, 'cp', None)
    rep_spec = P()

    def local_fn(u_in, seg_ids, grad_h, conv_w, conv_b, a_gate_w, a_gate_b, x_gate_w, x_gate_b, lam_param):
        n_batch, n_tok, n_width = u_in.shape
        n_heads, block_w, _ = a_gate_w.shape
        has_prev = lax.axis_index('cp') > 0
        halo_seg = lax.ppermute(seg_ids[:, n_tok - HALO:], 'cp', to_next)
        seg_ext = jnp.concatenate([halo_seg, seg_ids], axis=1).T
        ext_ok = (jnp.arange(n_tok + HALO) >= HALO) | has_prev
        masks = []
        for tap in range(1, CONV):
            tap_ok = (seg_ext[HALO - tap:HALO - tap + n_tok] == seg_ext[HALO:]) & ext_ok[HALO - tap:HALO - tap + n_tok, None]
            masks.append(tap_ok.astype(jnp.float32))
        masks.append((1.0 - masks[0]) * START_BIAS)
        masks = jnp.broadcast_to(jnp.stack(masks)[..., None], (HALO + 1, n_tok, n_batch, LANES))
        log_rate = -8.0 * jax.nn.softplus(-lam_param)
        par = jnp.concatenate([conv_w, conv_b[None], a_gate_b[None], x_gate_b[None], log_rate[None], log_rate[None] * LOG2E,
                               jnp.zeros((N_PAR - 9, n_width), jnp.float32)], axis=0)

        def now(step):
            return jnp.minimum(step, n_heads - 1)

        def late(step):
            return jnp.clip(step - LAG, 0, n_heads - 1)

        def blk_row(at):
            return pl.BlockSpec((n_batch, n_tok, block_w), lambda s: (0, 0, at(s)))

        tail_spec = pl.BlockSpec((n_batch, BLOCK, block_w), lambda s: (0, n_tok // BLOCK - 1, now(s + 1)))

        def mat_spec(at):
            return pl.BlockSpec((1, block_w, block_w), lambda s: (at(s), 0, 0))

        def par_spec(at):
            return pl.BlockSpec((N_PAR, block_w), lambda s: (0, at(s)))

        mask_spec = pl.BlockSpec((HALO + 1, n_tok, n_batch, LANES), lambda s: (0, 0, 0, 0), pipeline_mode=pl.Buffered(1))
        f32_slots = pltpu.VMEM((SLOTS, n_tok, n_batch, block_w), jnp.float32)
        f32_scr = pltpu.VMEM((n_tok, n_batch, block_w), jnp.float32)
        bf_scr = pltpu.VMEM((n_tok, n_batch, block_w), jnp.bfloat16)
        wire = pltpu.VMEM((n_heads, GROUP * PITCH, LANES), jnp.float32)
        half_wire = pltpu.VMEM((n_heads, GROUP * IN_ROWS, LANES), jnp.float32)
        sems = pltpu.SemaphoreType.DMA((n_heads,))

        item_f32 = functools.partial(pltpu.VMEM, dtype=jnp.float32)
        n_sems = 12
        du_time, grads = pl.pallas_call(
            functools.partial(fused_kernel, n_dev, n_heads), grid=(n_heads + LAG + AFTER[STAGES],),
            in_specs=[blk_row(now), tail_spec, blk_row(now), mask_spec, mat_spec(now), mat_spec(now),
                      mat_spec(late), mat_spec(late), par_spec(now), par_spec(late)],
            out_specs=[pl.BlockSpec(memory_space=pl.ANY)] * 2,
            out_shape=[jax.ShapeDtypeStruct((n_tok, n_batch, n_width), jnp.bfloat16),
                       jax.ShapeDtypeStruct((2, n_heads + 1, block_w, block_w), jnp.float32)],
            scratch_shapes=[pltpu.VMEM((SLOTS, n_tok + HALO, n_batch, block_w), jnp.float32)] + [f32_slots] * 7
            + [pltpu.VMEM((SLOTS, n_tok, n_batch, block_w), jnp.bfloat16), f32_scr, f32_scr, bf_scr, bf_scr] + [wire] * 2 + [half_wire] * 3
            + [item_f32((EDGE_SLOTS, HALO, n_batch, block_w))] * 2
            + [item_f32((PART_SLOTS, 2, block_w, block_w)), item_f32((FIRST_SLOTS, block_w, block_w)),
               item_f32((RECV_SLOTS, block_w // 2, block_w)), item_f32((RECV_SLOTS, block_w // 4, block_w)),
               item_f32((RECV_SLOTS, 3, block_w // 16, block_w)), item_f32((OWN_SLOTS, block_w, block_w)),
               item_f32((block_w, block_w)), item_f32((N_VEC, block_w)),
               pltpu.VMEM((EDGE_SLOTS, n_tok, n_batch, block_w), jnp.bfloat16)]
            + [item_f32((EDGE_SLOTS, HALO, n_batch, block_w))] * 2 + [item_f32((EDGE_IN, HALO, n_batch, block_w))]
            + [sems] * 2 + [pltpu.SemaphoreType.DMA((DEPTH - 1, n_heads))] * 2 + [sems] * 2 + [pltpu.SemaphoreType.DMA((EDGE_SLOTS,))] * 2
            + [pltpu.SemaphoreType.DMA((n_sems, OWN_SLOTS))] * 2
            + [pltpu.SemaphoreType.DMA((count,)) for count in (EDGE_SLOTS, EDGE_IN, EDGE_SLOTS, OWN_SLOTS)],
            compiler_params=pltpu.CompilerParams(vmem_limit_bytes=67043328, has_side_effects=True), name='fused_pass',
        )(u_in, u_in, grad_h, masks, a_gate_w, x_gate_w, a_gate_w, x_gate_w, par, par)
        vecs = grads[0, n_heads, :n_heads * N_VEC].reshape(n_heads, N_VEC, block_w)
        vecs = jnp.swapaxes(vecs, 0, 1).reshape(N_VEC, n_width)
        g_lam = 8.0 * jax.nn.sigmoid(-lam_param) * vecs[GLAM]
        return (jnp.swapaxes(du_time, 0, 1), vecs[GW:GW + CONV], vecs[GBC], grads[0, :n_heads], vecs[GBA],
                grads[1, :n_heads], vecs[GBI], g_lam)

    return jax.shard_map(local_fn, mesh=mesh,
                         in_specs=(seq_spec, P(None, 'cp'), seq_spec, rep_spec, rep_spec, rep_spec,
                                   rep_spec, rep_spec, rep_spec, rep_spec),
                         out_specs=(seq_spec,) + (rep_spec,) * 7, check_vma=False)
```

```python
import functools

import jax
import jax.numpy as jnp
from jax import lax
from jax.experimental import pallas as pl
from jax.experimental.pallas import tpu as pltpu
from jax.sharding import PartitionSpec as P

CONV = 4
HALO = CONV - 1
LOG2E = 1.4426950408889634
LN2 = 0.6931471805599453
START_BIAS = -1e4
LANES = 128
STEPS = 16
BLOCK = 16
LAG = 3
SLOTS = LAG + 1
GROUP, DEPTH = 8, 4
SUM_ROWS, IN_ROWS = 12, 8
PITCH = 16
PART_SLOTS, RECV_SLOTS, OWN_SLOTS, EDGE_SLOTS, EDGE_IN = 6, 4, 8, 4, 8
STAGES, FIRST_SLOTS = 8, 4
AFTER = (0, 1, 2, 3, 4, 5, 6, 7, 8)
MESH = pl.DeviceIdType.MESH

W0, BC, BA, BI, KL, KE = 0, 4, 5, 6, 7, 8
N_PAR = 16
GW, GBC, GBA, GBI, GLAM = 0, 4, 5, 6, 7
N_VEC = 8


def sigmoid_of(pre):
    root = lax.rsqrt(1.0 + jnp.exp2(pre * (-LOG2E)))
    return root * root


def decay_of(gate_r, par_ke, bias):
    log_two = gate_r * par_ke + bias
    decay = jnp.exp2(log_two)
    square = decay * decay
    gap = jnp.tanh(log_two * (-LN2)) * (1.0 + square)
    inv_root = lax.rsqrt(gap)
    return decay, gap * inv_root, square * inv_root * inv_root


def fold_rows(arr):
    return arr[:8] + arr[8:]


def dot_nn(lhs, rhs):
    return lax.dot_general(lhs, rhs, (((1,), (0,)), ((), ())), preferred_element_type=jnp.float32)


def dot_nt(lhs, rhs):
    return lax.dot_general(lhs, rhs, (((1,), (1,)), ((), ())), preferred_element_type=jnp.float32)


def dot_tn(lhs, rhs):
    return lax.dot_general(lhs, rhs, (((0,), (0,)), ((), ())), preferred_element_type=jnp.float32)


def fused_kernel(n_dev, n_heads,
                 u_ref, tail_ref, gh_ref, seg_ref, wa_ref, wi_ref, wa2_ref, wi2_ref, par_ref, par2_ref,
                 du_ref, grad_ref,
                 u_s, c_s, r_s, i_s, a_s, m_s, e_s, g_s, cb_s, h_scr, d_scr, ga_scr, gi_scr,
                 send, recv, group, resp, carry, halo_out, halo_in, mask_ref, seg_in, part, got0, got1, got2, got3, own, vec_all, vec_ref, du_s, tail_s, edge_out, edge_in,
                 send_sem, recv_sem, group_ssem, group_rsem, give_sem, take_sem, halo_ssem, halo_rsem, seg_sem, sum_ssem, sum_rsem, edge_ssem, edge_rsem, du_sem, put_sem):
    n_batch, n_tok, width = u_ref.shape
    step_id = pl.program_id(0)
    me = lax.axis_index('cp')
    rows = 256
    core = lax.rem(me, 2)
    x_at = lax.rem(me // 2, 2)
    y_at = lax.rem(me // 4, 2)
    z_at = me // GROUP
    place = lax.rem(me, GROUP)
    partner = me + 1 - 2 * core
    x_peer = me + 2 - 4 * x_at
    y_peer = me + 4 - 8 * y_at
    bit1 = x_at + core * (y_at - x_at)
    bit2 = y_at + core * (x_at - y_at)
    peer1 = x_peer + core * (y_peer - x_peer)
    peer2 = y_peer + core * (x_peer - y_peer)
    half_rows, quarter_rows = width // 2, width // 4
    piece = width // 16
    base1 = bit1 * half_rows
    base2 = base1 + bit2 * quarter_rows

    def row_range(start, count):
        return pl.ds(pl.multiple_of(start, count), count)

    def sum_copies(stage, item):
        p_at, r_at, o_at, s_at, f_at = (lax.rem(item, n) for n in (PART_SLOTS, RECV_SLOTS, OWN_SLOTS, OWN_SLOTS, FIRST_SLOTS))

        def one(index, src, dst, dev):
            return pltpu.make_async_remote_copy(src_ref=src, dst_ref=dst, send_sem=sum_ssem.at[index, s_at],
                                                recv_sem=sum_rsem.at[index, s_at], device_id=(dev,), device_id_type=MESH)

        def z_peer(k):
            z_to = lax.rem(z_at + k, 4)
            return z_to, z_to * GROUP + place

        if stage == 0:
            return [one(0, part.at[p_at, 1 - core], got0.at[f_at], partner)]
        if stage == 1:
            return [one(1, part.at[p_at, core, row_range((1 - bit1) * half_rows, half_rows)], got1.at[r_at], peer1)]
        if stage == 2:
            return [one(2, part.at[p_at, core, row_range(base1 + (1 - bit2) * quarter_rows, quarter_rows)], got2.at[r_at], peer2)]
        if stage == 3:
            return [one(2 + k, part.at[p_at, core, row_range(base2 + z_peer(k)[0] * piece, piece)], got3.at[r_at, k - 1], z_peer(k)[1])
                    for k in (1, 2, 3)]
        if stage == 4:
            mine = own.at[o_at, row_range(base2 + z_at * piece, piece)]
            return [one(5 + k, mine, mine, z_peer(k)[1]) for k in (1, 2, 3)]
        if stage == 5:
            mine = own.at[o_at, row_range(base2, quarter_rows)]
            return [one(9, mine, mine, peer2)]
        if stage == 6:
            mine = own.at[o_at, row_range(base1, half_rows)]
            return [one(10, mine, mine, peer1)]
        return [one(11, own.at[o_at], grad_ref.at[core, item], partner)]

    def put_copy(item):
        slot = lax.rem(item, OWN_SLOTS)
        return pltpu.make_async_copy(own.at[slot], grad_ref.at[core, item], put_sem.at[slot])

    def sum_stage(stage, item):
        p_at, r_at, o_at = (lax.rem(item, n) for n in (PART_SLOTS, RECV_SLOTS, OWN_SLOTS))
        for copy in sum_copies(stage - 1, item):
            copy.wait_recv()
            copy.wait_send()
        if stage == 1:
            part[p_at, core] = part[p_at, core] + got0[lax.rem(item, FIRST_SLOTS)]
        if stage == 2:
            at = row_range(base1, half_rows)
            part[p_at, core, at] = part[p_at, core, at] + got1[r_at]
        if stage == 3:
            at = row_range(base2, quarter_rows)
            part[p_at, core, at] = part[p_at, core, at] + got2[r_at]
        if stage == 4:
            at = row_range(base2 + z_at * piece, piece)
            own[o_at, at] = (part[p_at, core, at] + got3[r_at, 0]) + (got3[r_at, 1] + got3[r_at, 2])
        if stage == STAGES:
            put_copy(item).wait()
        else:
            for copy in sum_copies(stage, item):
                copy.start()
        if stage == STAGES - 1:
            put_copy(item).start()

    def edge_copy(head):
        slot, to = lax.rem(head, EDGE_SLOTS), lax.rem(head, EDGE_IN)
        return pltpu.make_async_remote_copy(src_ref=edge_out.at[slot], dst_ref=edge_in.at[to], send_sem=edge_ssem.at[slot],
                                            recv_sem=edge_rsem.at[to], device_id=(lax.rem(me + n_dev - 1, n_dev),), device_id_type=MESH)

    def du_copy(head):
        slot = lax.rem(head, EDGE_SLOTS)
        return pltpu.make_async_copy(du_s.at[slot], du_ref.at[:, :, pl.ds(pl.multiple_of(head * width, width), width)], du_sem.at[slot])

    def block_of(index, pitch, count):
        return pl.ds(pl.multiple_of(index * pitch, pitch), count)

    def spread(src, dst, out_sem, in_sem, head, pitch, count):
        def one(k, _):
            to = lax.rem(place + k, GROUP)
            pltpu.make_async_remote_copy(
                src_ref=src.at[head, block_of(to, pitch, count)], dst_ref=dst.at[head, block_of(place, pitch, count)],
                send_sem=out_sem.at[head], recv_sem=in_sem.at[head],
                device_id=(z_at * GROUP + to,), device_id_type=MESH).start()
            return 0
        lax.fori_loop(1, GROUP, one, 0, unroll=True)
        own_rows = block_of(place, pitch, pitch)
        dst[head, own_rows, :] = src[head, own_rows, :]

    def settle(buf, sem, head, total):
        all_rows = buf.at[head, pl.ds(0, total)]
        pltpu.make_async_copy(all_rows, all_rows, sem.at[head]).wait()

    def rows_of(buf, head, index, quantity):
        start = index * PITCH + 4 * quantity
        return buf[head, start:start + 4, :]

    def halo_copy(head):
        slot = lax.rem(head, EDGE_SLOTS)
        return pltpu.make_async_remote_copy(src_ref=halo_out.at[slot], dst_ref=halo_in.at[slot], send_sem=halo_ssem.at[slot],
                                            recv_sem=halo_rsem.at[slot], device_id=(lax.rem(me + 1, n_dev),), device_id_type=MESH)

    def halo_send(head, src_ref):
        last = jnp.swapaxes(src_ref[:, src_ref.shape[1] - BLOCK:, :].astype(jnp.float32), 0, 1)
        halo_out[lax.rem(head, EDGE_SLOTS)] = last[BLOCK - HALO:]
        halo_copy(head).start()

    @pl.when(step_id == 0)
    def _begin():
        vec_all[...] = jnp.zeros_like(vec_all)
        seg_copy = pltpu.make_async_remote_copy(src_ref=seg_ref.at[pl.ds(n_tok - HALO, HALO)], dst_ref=seg_in, send_sem=seg_sem.at[0],
                                                recv_sem=seg_sem.at[1], device_id=(lax.rem(me + 1, n_dev),), device_id_type=MESH)
        seg_copy.start()
        halo_send(0, u_ref)
        seg_copy.wait_recv()
        seg_copy.wait_send()
        has_prev = jnp.where(me > 0, 1.0, 0.0)
        for tap in range(1, CONV):
            mask_ref[tap - 1, tap:] = jnp.where(seg_ref[tap:] == seg_ref[:n_tok - tap], 1.0, 0.0)
            mask_ref[tap - 1, :tap] = jnp.where(seg_ref[:tap] == seg_in[HALO - tap:], 1.0, 0.0) * has_prev
        mask_ref[HALO] = (1.0 - mask_ref[0]) * START_BIAS

    def group_copies(head):
        mine = group.at[head, block_of(z_at, PITCH, SUM_ROWS)]
        return [pltpu.make_async_remote_copy(src_ref=mine, dst_ref=mine, send_sem=group_ssem.at[k, head], recv_sem=group_rsem.at[k, head],
                                             device_id=(lax.rem(z_at + 1 + k, DEPTH) * GROUP + place,), device_id_type=MESH)
                for k in range(DEPTH - 1)]

    def combine(head):
        for copy in group_copies(head):
            copy.wait_recv()
            copy.wait_send()
        state = jnp.zeros((4, LANES), jnp.float32)
        adj = jnp.zeros((4, LANES), jnp.float32)
        for index in range(DEPTH - 1):
            step_state = rows_of(group, head, index, 0) * state + rows_of(group, head, index, 1)
            state = jnp.where(index < z_at, step_state, state)
            other = DEPTH - 1 - index
            step_adj = rows_of(group, head, other, 0) * adj + rows_of(group, head, other, 2)
            adj = jnp.where(other > z_at, step_adj, adj)
        for index in range(GROUP):
            other = GROUP - 1 - index
            resp[head, index * IN_ROWS:index * IN_ROWS + 4, :] = state
            resp[head, other * IN_ROWS + 4:other * IN_ROWS + 8, :] = adj
            state = rows_of(recv, head, index, 0) * state + rows_of(recv, head, index, 1)
            adj = rows_of(recv, head, other, 0) * adj + rows_of(recv, head, other, 2)
        spread(resp, carry, give_sem, take_sem, head, IN_ROWS, IN_ROWS)

    def put_rows(head, quantity, half, val):
        for high in range(2):
            send.at[head][pl.ds(4 * quantity + 2 * high + half, GROUP, stride=PITCH), :] = val[high * GROUP:(high + 1) * GROUP]

    def take_rows(head, quantity, half):
        return jnp.concatenate([carry.at[head][pl.ds(4 * quantity + 2 * high + half, GROUP, stride=IN_ROWS), :] for high in range(2)], axis=0)

    @pl.when(step_id < n_heads)
    def _first():
        head = step_id
        slot = lax.rem(step_id, SLOTS)
        halo_copy(head).wait_recv()
        halo_copy(head).wait_send()
        u_s[slot, :HALO] = halo_in[lax.rem(head, EDGE_SLOTS)]

        @pl.when(head + 1 < n_heads)
        def _next_halo():
            halo_send(head + 1, tail_ref)

        for start in range(0, n_tok, BLOCK):
            u_s[slot, HALO + start:HALO + start + BLOCK] = jnp.swapaxes(u_ref[:, start:start + BLOCK, :].astype(jnp.float32), 0, 1)
            for tok in range(start, start + BLOCK):
                for lane in range(0, width, LANES):
                    cols = slice(lane, lane + LANES)
                    acc = par_ref[BC:BC + 1, cols] + par_ref[W0:W0 + 1, cols] * u_s[slot, tok + HALO, :, cols]
                    for tap in range(1, CONV):
                        acc = acc + par_ref[W0 + tap:W0 + tap + 1, cols] * (mask_ref[tap - 1, tok] * u_s[slot, tok + HALO - tap, :, cols])
                    c_s[slot, tok, :, cols] = acc
                    cb_s[slot, tok, :, cols] = acc.astype(jnp.bfloat16)
            g_s[slot, start:start + BLOCK] = jnp.swapaxes(gh_ref[:, start:start + BLOCK, :], 0, 1)
            part_c = cb_s[slot, start:start + BLOCK].reshape(rows, width)
            r_s[slot, start:start + BLOCK] = dot_nn(part_c, wa_ref[0]).reshape(BLOCK, n_batch, width)
            i_s[slot, start:start + BLOCK] = dot_nn(part_c, wi_ref[0]).reshape(BLOCK, n_batch, width)

        for half in range(width // LANES):
            cols = slice(half * LANES, (half + 1) * LANES)

            def fwd_body(chunk, run):
                state, prod = run
                base = chunk * STEPS
                for step in range(STEPS):
                    tok = base + step
                    gate_r = sigmoid_of(r_s[slot, tok, :, cols] + par_ref[BA:BA + 1, cols])
                    gate_i = sigmoid_of(i_s[slot, tok, :, cols] + par_ref[BI:BI + 1, cols])
                    decay, mult, ratio = decay_of(gate_r, par_ref[KE:KE + 1, cols], mask_ref[HALO, tok])
                    r_s[slot, tok, :, cols] = gate_r
                    i_s[slot, tok, :, cols] = gate_i
                    a_s[slot, tok, :, cols] = decay
                    m_s[slot, tok, :, cols] = mult
                    e_s[slot, tok, :, cols] = ratio
                    state = decay * state + mult * (gate_i * c_s[slot, tok, :, cols])
                    prod = decay * prod
                return state, prod

            zero = jnp.zeros((n_batch, LANES), jnp.float32)
            state, prod = lax.fori_loop(0, n_tok // STEPS, fwd_body, (zero, zero + 1.0))

            put_rows(head, 0, half, prod)
            put_rows(head, 1, half, state)

        def adj_body(chunk, adj):
            base = n_tok - STEPS - chunk * STEPS
            for step in reversed(range(STEPS)):
                tok = base + step
                adj = a_s[slot, tok] * (g_s[slot, tok] + adj)
            return adj

        first = lax.fori_loop(0, n_tok // STEPS, adj_body, jnp.zeros((n_batch, width), jnp.float32))
        for half in range(width // LANES):
            put_rows(head, 2, half, first[:, half * LANES:(half + 1) * LANES])
        spread(send, recv, send_sem, recv_sem, head, PITCH, SUM_ROWS)

    @pl.when((step_id >= 2) & (step_id <= n_heads + 1))
    def _combine():
        combine(step_id - 2)

    @pl.when((step_id >= 1) & (step_id <= n_heads))
    def _group():
        head = step_id - 1
        settle(recv, recv_sem, head, (GROUP - 1) * SUM_ROWS)
        prod = jnp.ones((4, LANES), jnp.float32)
        state = jnp.zeros((4, LANES), jnp.float32)
        adj = jnp.zeros((4, LANES), jnp.float32)
        for index in range(GROUP):
            decay = rows_of(recv, head, index, 0)
            state = decay * state + rows_of(recv, head, index, 1)
            prod = decay * prod
            other = GROUP - 1 - index
            adj = rows_of(recv, head, other, 0) * adj + rows_of(recv, head, other, 2)
        mine = block_of(z_at, PITCH, PITCH)
        group[head, mine, :] = jnp.concatenate([prod, state, adj, jnp.zeros_like(adj)], axis=0)
        for copy in group_copies(head):
            copy.start()

    for stage in reversed(range(1, STAGES + 1)):
        item_of = step_id - LAG - AFTER[stage]

        @pl.when((item_of >= 0) & (item_of < n_heads))
        def _sum(stage=stage, item_of=item_of):
            sum_stage(stage, item_of)

        @pl.when(item_of == n_heads - 1)
        def _sum_vectors(stage=stage):
            sum_stage(stage, n_heads)

    head_done = step_id - LAG - 3

    @pl.when((head_done >= 0) & (head_done < n_heads))
    def _stored():
        du_copy(head_done).wait()

    head_edge = step_id - LAG - 2

    @pl.when((head_edge >= 0) & (head_edge < n_heads))
    def _edge():
        slot = lax.rem(head_edge, EDGE_SLOTS)
        edge_copy(head_edge).wait_recv()
        edge_copy(head_edge).wait_send()
        du_s[slot, n_tok - HALO:] = (tail_s[slot] + edge_in[lax.rem(head_edge, EDGE_IN)]).astype(jnp.bfloat16)
        du_copy(head_edge).start()

    @pl.when((step_id >= LAG) & (step_id < n_heads + LAG))
    def _second():
        head = step_id - LAG
        slot = lax.rem(step_id - LAG, SLOTS)
        e_at = lax.rem(head, EDGE_SLOTS)
        settle(carry, take_sem, head, (GROUP - 1) * IN_ROWS)

        def state_body(chunk, state):
            base = chunk * STEPS
            for step in range(STEPS):
                tok = base + step
                h_scr[tok] = state
                state = a_s[slot, tok] * state + m_s[slot, tok] * (i_s[slot, tok] * c_s[slot, tok])
            return state

        state_in = [take_rows(head, 0, half) for half in range(width // LANES)]
        lax.fori_loop(0, n_tok // STEPS, state_body, jnp.concatenate(state_in, axis=1))

        for half in range(width // LANES):
            cols = slice(half * LANES, (half + 1) * LANES)
            zero8 = jnp.zeros((8, LANES), jnp.float32)

            def bwd_body(chunk, run):
                adj_next, sum_a, sum_i, sum_l = run
                base = n_tok - STEPS - chunk * STEPS
                for step in reversed(range(STEPS)):
                    tok = base + step
                    gate_r = r_s[slot, tok, :, cols]
                    gate_i = i_s[slot, tok, :, cols]
                    conv_c = c_s[slot, tok, :, cols]
                    adj = g_s[slot, tok, :, cols] + adj_next
                    adj_next = a_s[slot, tok, :, cols] * adj
                    direct = adj * m_s[slot, tok, :, cols] * gate_i
                    d_input = direct * conv_c
                    d_pre_i = d_input * (1.0 - gate_i)
                    d_log = adj_next * h_scr[tok, :, cols] - d_input * e_s[slot, tok, :, cols]
                    d_log_r = d_log * gate_r
                    d_pre_a = d_log_r * (par2_ref[KL:KL + 1, cols] * (1.0 - gate_r))
                    sum_l = sum_l + fold_rows(d_log_r)
                    sum_a = sum_a + fold_rows(d_pre_a)
                    sum_i = sum_i + fold_rows(d_pre_i)
                    d_scr[tok, :, cols] = direct
                    ga_scr[tok, :, cols] = d_pre_a.astype(jnp.bfloat16)
                    gi_scr[tok, :, cols] = d_pre_i.astype(jnp.bfloat16)
                return adj_next, sum_a, sum_i, sum_l

            adj_in = take_rows(head, 1, half)
            _, sum_a, sum_i, sum_l = lax.fori_loop(0, n_tok // STEPS, bwd_body, (adj_in, zero8, zero8, zero8))
            vec_ref[GBA:GBA + 1, cols] = jnp.sum(sum_a, axis=0, keepdims=True)
            vec_ref[GBI:GBI + 1, cols] = jnp.sum(sum_i, axis=0, keepdims=True)
            vec_ref[GLAM:GLAM + 1, cols] = jnp.sum(sum_l, axis=0, keepdims=True)

        p_at = lax.rem(head, PART_SLOTS)
        all_c = cb_s[slot].reshape(n_tok * n_batch, width)
        part[p_at, 0] = dot_tn(all_c, ga_scr[...].reshape(n_tok * n_batch, width))
        part[p_at, 1] = dot_tn(all_c, gi_scr[...].reshape(n_tok * n_batch, width))

        halves = width // LANES
        sums = [[jnp.zeros((8, LANES), jnp.float32)] * (CONV + 1) for _ in range(halves)]
        ahead = [[jnp.zeros((n_batch, LANES), jnp.float32)] * HALO for _ in range(halves)]
        for start in reversed(range(0, n_tok, BLOCK)):
            toks = slice(start, start + BLOCK)
            back = dot_nt(ga_scr[toks].reshape(rows, width), wa2_ref[0]) + dot_nt(gi_scr[toks].reshape(rows, width), wi2_ref[0])
            d_scr[toks] = d_scr[toks] + back.reshape(BLOCK, n_batch, width)
            for half in range(halves):
                cols = slice(half * LANES, (half + 1) * LANES)
                tot, nxt = sums[half], ahead[half]
                for tok in reversed(range(start, start + BLOCK)):
                    d_conv = d_scr[tok, :, cols]
                    tot[CONV] = tot[CONV] + fold_rows(d_conv)
                    masked = [d_conv] + [mask_ref[tap - 1, tok] * d_conv for tap in range(1, CONV)]
                    for tap in range(CONV):
                        tot[tap] = tot[tap] + fold_rows(masked[tap] * u_s[slot, tok + HALO - tap, :, cols])
                    terms = [par2_ref[W0 + tap:W0 + tap + 1, cols] * masked[tap] for tap in range(CONV)]
                    d_u = nxt[0] + terms[0]
                    du_s[e_at, tok, :, cols] = d_u.astype(jnp.bfloat16)
                    if tok >= n_tok - HALO:
                        tail_s[e_at, tok - n_tok + HALO, :, cols] = d_u
                    nxt = [nxt[1] + terms[1], nxt[2] + terms[2], terms[3]]
                ahead[half] = nxt
        for half in range(halves):
            cols = slice(half * LANES, (half + 1) * LANES)
            for row in range(CONV + 1):
                vec_ref[GW + row:GW + row + 1, cols] = jnp.sum(sums[half][row], axis=0, keepdims=True)
            for row in range(HALO):
                edge_out[e_at, HALO - 1 - row, :, cols] = ahead[half][row]
        edge_copy(head).start()
        vec_all[pl.ds(pl.multiple_of(head * N_VEC, N_VEC), N_VEC), :] = vec_ref[...]

    item_new = step_id - LAG

    @pl.when((item_new >= 0) & (item_new < n_heads))
    def _share():
        for copy in sum_copies(0, item_new):
            copy.start()

    @pl.when(item_new == n_heads - 1)
    def _share_vectors():
        p_at = n_heads % PART_SLOTS
        part[p_at, 0] = vec_all[...]
        part[p_at, 1] = jnp.zeros_like(vec_all)
        for copy in sum_copies(0, n_heads):
            copy.start()

    @pl.when(step_id == n_heads - 1 + LAG)
    def _drain():
        def one(head, _):
            settle(send, send_sem, head, (GROUP - 1) * SUM_ROWS)
            settle(resp, give_sem, head, (GROUP - 1) * IN_ROWS)
            return 0
        lax.fori_loop(0, n_heads, one, 0)


def solution(mesh):
    n_dev = mesh.shape['cp']
    seq_spec = P(None, 'cp', None)
    rep_spec = P()

    def local_fn(u_in, seg_ids, grad_h, conv_w, conv_b, a_gate_w, a_gate_b, x_gate_w, x_gate_b, lam_param):
        n_batch, n_tok, n_width = u_in.shape
        n_heads, block_w, _ = a_gate_w.shape
        seg_time = jnp.broadcast_to(seg_ids.T[:, :, None], (n_tok, n_batch, LANES))
        log_rate = -8.0 * jax.nn.softplus(-lam_param)
        par = jnp.concatenate([conv_w, conv_b[None], a_gate_b[None], x_gate_b[None], log_rate[None], log_rate[None] * LOG2E,
                               jnp.zeros((N_PAR - 9, n_width), jnp.float32)], axis=0)

        def now(step):
            return jnp.minimum(step, n_heads - 1)

        def late(step):
            return jnp.clip(step - LAG, 0, n_heads - 1)

        def blk_row(at):
            return pl.BlockSpec((n_batch, n_tok, block_w), lambda s: (0, 0, at(s)))

        tail_spec = pl.BlockSpec((n_batch, BLOCK, block_w), lambda s: (0, n_tok // BLOCK - 1, now(s + 1)))

        def mat_spec(at):
            return pl.BlockSpec((1, block_w, block_w), lambda s: (at(s), 0, 0))

        def par_spec(at):
            return pl.BlockSpec((N_PAR, block_w), lambda s: (0, at(s)))

        seg_spec = pl.BlockSpec((n_tok, n_batch, LANES), lambda s: (0, 0, 0), pipeline_mode=pl.Buffered(1))
        f32_slots = pltpu.VMEM((SLOTS, n_tok, n_batch, block_w), jnp.float32)
        f32_scr = pltpu.VMEM((n_tok, n_batch, block_w), jnp.float32)
        bf_scr = pltpu.VMEM((n_tok, n_batch, block_w), jnp.bfloat16)
        wire = pltpu.VMEM((n_heads, GROUP * PITCH, LANES), jnp.float32)
        half_wire = pltpu.VMEM((n_heads, GROUP * IN_ROWS, LANES), jnp.float32)
        sems = pltpu.SemaphoreType.DMA((n_heads,))

        item_f32 = functools.partial(pltpu.VMEM, dtype=jnp.float32)
        n_sems = 12
        du_time, grads = pl.pallas_call(
            functools.partial(fused_kernel, n_dev, n_heads), grid=(n_heads + LAG + AFTER[STAGES],),
            in_specs=[blk_row(now), tail_spec, blk_row(now), seg_spec, mat_spec(now), mat_spec(now),
                      mat_spec(late), mat_spec(late), par_spec(now), par_spec(late)],
            out_specs=[pl.BlockSpec(memory_space=pl.ANY)] * 2,
            out_shape=[jax.ShapeDtypeStruct((n_tok, n_batch, n_width), jnp.bfloat16),
                       jax.ShapeDtypeStruct((2, n_heads + 1, block_w, block_w), jnp.float32)],
            scratch_shapes=[pltpu.VMEM((SLOTS, n_tok + HALO, n_batch, block_w), jnp.float32)] + [f32_slots] * 7
            + [pltpu.VMEM((SLOTS, n_tok, n_batch, block_w), jnp.bfloat16), f32_scr, f32_scr, bf_scr, bf_scr] + [wire] * 2 + [half_wire] * 3
            + [item_f32((EDGE_SLOTS, HALO, n_batch, block_w))] * 2
            + [item_f32((HALO + 1, n_tok, n_batch, LANES)), pltpu.VMEM((HALO, n_batch, LANES), jnp.int32)]
            + [item_f32((PART_SLOTS, 2, block_w, block_w)), item_f32((FIRST_SLOTS, block_w, block_w)),
               item_f32((RECV_SLOTS, block_w // 2, block_w)), item_f32((RECV_SLOTS, block_w // 4, block_w)),
               item_f32((RECV_SLOTS, 3, block_w // 16, block_w)), item_f32((OWN_SLOTS, block_w, block_w)),
               item_f32((block_w, block_w)), item_f32((N_VEC, block_w)),
               pltpu.VMEM((EDGE_SLOTS, n_tok, n_batch, block_w), jnp.bfloat16)]
            + [item_f32((EDGE_SLOTS, HALO, n_batch, block_w))] * 2 + [item_f32((EDGE_IN, HALO, n_batch, block_w))]
            + [sems] * 2 + [pltpu.SemaphoreType.DMA((DEPTH - 1, n_heads))] * 2 + [sems] * 2 + [pltpu.SemaphoreType.DMA((EDGE_SLOTS,))] * 2
            + [pltpu.SemaphoreType.DMA((2,))]
            + [pltpu.SemaphoreType.DMA((n_sems, OWN_SLOTS))] * 2
            + [pltpu.SemaphoreType.DMA((count,)) for count in (EDGE_SLOTS, EDGE_IN, EDGE_SLOTS, OWN_SLOTS)],
            compiler_params=pltpu.CompilerParams(vmem_limit_bytes=67043328, has_side_effects=True), name='fused_pass',
        )(u_in, u_in, grad_h, seg_time, a_gate_w, x_gate_w, a_gate_w, x_gate_w, par, par)
        vecs = grads[0, n_heads, :n_heads * N_VEC].reshape(n_heads, N_VEC, block_w)
        vecs = jnp.swapaxes(vecs, 0, 1).reshape(N_VEC, n_width)
        g_lam = 8.0 * jax.nn.sigmoid(-lam_param) * vecs[GLAM]
        return (jnp.swapaxes(du_time, 0, 1), vecs[GW:GW + CONV], vecs[GBC], grads[0, :n_heads], vecs[GBA],
                grads[1, :n_heads], vecs[GBI], g_lam)

    return jax.shard_map(local_fn, mesh=mesh,
                         in_specs=(seq_spec, P(None, 'cp'), seq_spec, rep_spec, rep_spec, rep_spec,
                                   rep_spec, rep_spec, rep_spec, rep_spec),
                         out_specs=(seq_spec,) + (rep_spec,) * 7, check_vma=False)
```

```python
import functools

import jax
import jax.numpy as jnp
from jax import lax
from jax.experimental import pallas as pl
from jax.experimental.pallas import tpu as pltpu
from jax.sharding import PartitionSpec as P

CONV = 4
HALO = CONV - 1
LOG2E = 1.4426950408889634
LN2 = 0.6931471805599453
START_BIAS = -1e4
LANES = 128
STEPS = 16
BLOCK = 16
LAG = 3
SLOTS = LAG + 1
GROUP, DEPTH = 8, 4
SUM_ROWS, IN_ROWS = 12, 8
PITCH = 16
PART_SLOTS, RECV_SLOTS, OWN_SLOTS, EDGE_SLOTS, EDGE_IN = 6, 4, 8, 4, 8
STAGES, FIRST_SLOTS = 8, 4
AFTER = (0, 1, 2, 3, 4, 5, 6, 7, 8)
MESH = pl.DeviceIdType.MESH

W0, BC, BA, BI, KL, KE = 0, 4, 5, 6, 7, 8
N_PAR = 9
GW, GBC, GBA, GBI, GLAM = 0, 4, 5, 6, 7
N_VEC = 8


def sigmoid_of(pre):
    root = lax.rsqrt(1.0 + jnp.exp2(pre * (-LOG2E)))
    return root * root


def decay_of(gate_r, par_ke, bias):
    log_two = gate_r * par_ke + bias
    decay = jnp.exp2(log_two)
    square = decay * decay
    gap = jnp.tanh(log_two * (-LN2)) * (1.0 + square)
    inv_root = lax.rsqrt(gap)
    return decay, gap * inv_root, square * inv_root * inv_root


def fold_rows(arr):
    return arr[:8] + arr[8:]


def dot_nn(lhs, rhs):
    return lax.dot_general(lhs, rhs, (((1,), (0,)), ((), ())), preferred_element_type=jnp.float32)


def dot_nt(lhs, rhs):
    return lax.dot_general(lhs, rhs, (((1,), (1,)), ((), ())), preferred_element_type=jnp.float32)


def dot_tn(lhs, rhs):
    return lax.dot_general(lhs, rhs, (((0,), (0,)), ((), ())), preferred_element_type=jnp.float32)


def fused_kernel(n_dev, n_heads,
                 u_ref, tail_ref, gh_ref, seg_ref, wa_ref, wi_ref, wa2_ref, wi2_ref, par_ref, par2_ref,
                 du_ref, grad_ref,
                 u_s, c_s, r_s, i_s, a_s, m_s, e_s, g_s, cb_s, h_scr, d_scr, ga_scr, gi_scr,
                 send, recv, group, resp, carry, halo_out, halo_in, mask_ref, seg_in, part, got0, got1, got2, got3, own, vec_all, vec_ref, du_s, tail_s, edge_out, edge_in,
                 send_sem, recv_sem, group_ssem, group_rsem, give_sem, take_sem, halo_ssem, halo_rsem, seg_sem, sum_ssem, sum_rsem, edge_ssem, edge_rsem, du_sem, put_sem):
    n_batch, n_tok, width = u_ref.shape
    step_id = pl.program_id(0)
    me = lax.axis_index('cp')
    rows = 256
    core = lax.rem(me, 2)
    x_at = lax.rem(me // 2, 2)
    y_at = lax.rem(me // 4, 2)
    z_at = me // GROUP
    place = lax.rem(me, GROUP)
    partner = me + 1 - 2 * core
    x_peer = me + 2 - 4 * x_at
    y_peer = me + 4 - 8 * y_at
    bit1 = x_at + core * (y_at - x_at)
    bit2 = y_at + core * (x_at - y_at)
    peer1 = x_peer + core * (y_peer - x_peer)
    peer2 = y_peer + core * (x_peer - y_peer)
    half_rows, quarter_rows = width // 2, width // 4
    piece = width // 16
    base1 = bit1 * half_rows
    base2 = base1 + bit2 * quarter_rows

    def row_range(start, count):
        return pl.ds(pl.multiple_of(start, count), count)

    def sum_copies(stage, item):
        p_at, r_at, o_at, s_at, f_at = (lax.rem(item, n) for n in (PART_SLOTS, RECV_SLOTS, OWN_SLOTS, OWN_SLOTS, FIRST_SLOTS))

        def one(index, src, dst, dev):
            return pltpu.make_async_remote_copy(src_ref=src, dst_ref=dst, send_sem=sum_ssem.at[index, s_at],
                                                recv_sem=sum_rsem.at[index, s_at], device_id=(dev,), device_id_type=MESH)

        def z_peer(k):
            z_to = lax.rem(z_at + k, 4)
            return z_to, z_to * GROUP + place

        if stage == 0:
            return [one(0, part.at[p_at, 1 - core], got0.at[f_at], partner)]
        if stage == 1:
            return [one(1, part.at[p_at, core, row_range((1 - bit1) * half_rows, half_rows)], got1.at[r_at], peer1)]
        if stage == 2:
            return [one(2, part.at[p_at, core, row_range(base1 + (1 - bit2) * quarter_rows, quarter_rows)], got2.at[r_at], peer2)]
        if stage == 3:
            return [one(2 + k, part.at[p_at, core, row_range(base2 + z_peer(k)[0] * piece, piece)], got3.at[r_at, k - 1], z_peer(k)[1])
                    for k in (1, 2, 3)]
        if stage == 4:
            mine = own.at[o_at, row_range(base2 + z_at * piece, piece)]
            return [one(5 + k, mine, mine, z_peer(k)[1]) for k in (1, 2, 3)]
        if stage == 5:
            mine = own.at[o_at, row_range(base2, quarter_rows)]
            return [one(9, mine, mine, peer2)]
        if stage == 6:
            mine = own.at[o_at, row_range(base1, half_rows)]
            return [one(10, mine, mine, peer1)]
        return [one(11, own.at[o_at], grad_ref.at[core, item], partner)]

    def put_copy(item):
        slot = lax.rem(item, OWN_SLOTS)
        return pltpu.make_async_copy(own.at[slot], grad_ref.at[core, item], put_sem.at[slot])

    def sum_stage(stage, item):
        p_at, r_at, o_at = (lax.rem(item, n) for n in (PART_SLOTS, RECV_SLOTS, OWN_SLOTS))
        for copy in sum_copies(stage - 1, item):
            copy.wait_recv()
            copy.wait_send()
        if stage == 1:
            part[p_at, core] = part[p_at, core] + got0[lax.rem(item, FIRST_SLOTS)]
        if stage == 2:
            at = row_range(base1, half_rows)
            part[p_at, core, at] = part[p_at, core, at] + got1[r_at]
        if stage == 3:
            at = row_range(base2, quarter_rows)
            part[p_at, core, at] = part[p_at, core, at] + got2[r_at]
        if stage == 4:
            at = row_range(base2 + z_at * piece, piece)
            own[o_at, at] = (part[p_at, core, at] + got3[r_at, 0]) + (got3[r_at, 1] + got3[r_at, 2])
        if stage == STAGES:
            put_copy(item).wait()
        else:
            for copy in sum_copies(stage, item):
                copy.start()
        if stage == STAGES - 1:
            put_copy(item).start()

    def edge_copy(head):
        slot, to = lax.rem(head, EDGE_SLOTS), lax.rem(head, EDGE_IN)
        return pltpu.make_async_remote_copy(src_ref=edge_out.at[slot], dst_ref=edge_in.at[to], send_sem=edge_ssem.at[slot],
                                            recv_sem=edge_rsem.at[to], device_id=(lax.rem(me + n_dev - 1, n_dev),), device_id_type=MESH)

    def du_copy(head):
        slot = lax.rem(head, EDGE_SLOTS)
        return pltpu.make_async_copy(du_s.at[slot], du_ref.at[:, :, pl.ds(pl.multiple_of(head * width, width), width)], du_sem.at[slot])

    def block_of(index, pitch, count):
        return pl.ds(pl.multiple_of(index * pitch, pitch), count)

    def spread(src, dst, out_sem, in_sem, head, pitch, count):
        def one(k, _):
            to = lax.rem(place + k, GROUP)
            pltpu.make_async_remote_copy(
                src_ref=src.at[head, block_of(to, pitch, count)], dst_ref=dst.at[head, block_of(place, pitch, count)],
                send_sem=out_sem.at[head], recv_sem=in_sem.at[head],
                device_id=(z_at * GROUP + to,), device_id_type=MESH).start()
            return 0
        lax.fori_loop(1, GROUP, one, 0, unroll=True)
        own_rows = block_of(place, pitch, pitch)
        dst[head, own_rows, :] = src[head, own_rows, :]

    def settle(buf, sem, head, total):
        all_rows = buf.at[head, pl.ds(0, total)]
        pltpu.make_async_copy(all_rows, all_rows, sem.at[head]).wait()

    def rows_of(buf, head, index, quantity):
        start = index * PITCH + 4 * quantity
        return buf[head, start:start + 4, :]

    def halo_copy(head):
        slot = lax.rem(head, EDGE_SLOTS)
        return pltpu.make_async_remote_copy(src_ref=halo_out.at[slot], dst_ref=halo_in.at[slot], send_sem=halo_ssem.at[slot],
                                            recv_sem=halo_rsem.at[slot], device_id=(lax.rem(me + 1, n_dev),), device_id_type=MESH)

    def halo_send(head, src_ref):
        last = jnp.swapaxes(src_ref[:, src_ref.shape[1] - BLOCK:, :].astype(jnp.float32), 0, 1)
        halo_out[lax.rem(head, EDGE_SLOTS)] = last[BLOCK - HALO:]
        halo_copy(head).start()

    @pl.when(step_id == 0)
    def _begin():
        vec_all[...] = jnp.zeros_like(vec_all)
        seg_copy = pltpu.make_async_remote_copy(src_ref=seg_ref.at[pl.ds(n_tok - HALO, HALO)], dst_ref=seg_in, send_sem=seg_sem.at[0],
                                                recv_sem=seg_sem.at[1], device_id=(lax.rem(me + 1, n_dev),), device_id_type=MESH)
        seg_copy.start()
        halo_send(0, u_ref)
        seg_copy.wait_recv()
        seg_copy.wait_send()
        has_prev = jnp.where(me > 0, 1.0, 0.0)
        for tap in range(1, CONV):
            mask_ref[tap - 1, tap:] = jnp.where(seg_ref[tap:] == seg_ref[:n_tok - tap], 1.0, 0.0)
            mask_ref[tap - 1, :tap] = jnp.where(seg_ref[:tap] == seg_in[HALO - tap:], 1.0, 0.0) * has_prev
        mask_ref[HALO] = (1.0 - mask_ref[0]) * START_BIAS

    def group_copies(head):
        mine = group.at[head, block_of(z_at, PITCH, SUM_ROWS)]
        return [pltpu.make_async_remote_copy(src_ref=mine, dst_ref=mine, send_sem=group_ssem.at[k, head], recv_sem=group_rsem.at[k, head],
                                             device_id=(lax.rem(z_at + 1 + k, DEPTH) * GROUP + place,), device_id_type=MESH)
                for k in range(DEPTH - 1)]

    def combine(head):
        for copy in group_copies(head):
            copy.wait_recv()
            copy.wait_send()
        state = jnp.zeros((4, LANES), jnp.float32)
        adj = jnp.zeros((4, LANES), jnp.float32)
        for index in range(DEPTH - 1):
            step_state = rows_of(group, head, index, 0) * state + rows_of(group, head, index, 1)
            state = jnp.where(index < z_at, step_state, state)
            other = DEPTH - 1 - index
            step_adj = rows_of(group, head, other, 0) * adj + rows_of(group, head, other, 2)
            adj = jnp.where(other > z_at, step_adj, adj)
        for index in range(GROUP):
            other = GROUP - 1 - index
            resp[head, index * IN_ROWS:index * IN_ROWS + 4, :] = state
            resp[head, other * IN_ROWS + 4:other * IN_ROWS + 8, :] = adj
            state = rows_of(recv, head, index, 0) * state + rows_of(recv, head, index, 1)
            adj = rows_of(recv, head, other, 0) * adj + rows_of(recv, head, other, 2)
        spread(resp, carry, give_sem, take_sem, head, IN_ROWS, IN_ROWS)

    def put_rows(head, quantity, half, val):
        for high in range(2):
            send.at[head][pl.ds(4 * quantity + 2 * high + half, GROUP, stride=PITCH), :] = val[high * GROUP:(high + 1) * GROUP]

    def take_rows(head, quantity, half):
        return jnp.concatenate([carry.at[head][pl.ds(4 * quantity + 2 * high + half, GROUP, stride=IN_ROWS), :] for high in range(2)], axis=0)

    @pl.when(step_id < n_heads)
    def _first():
        head = step_id
        slot = lax.rem(step_id, SLOTS)
        halo_copy(head).wait_recv()
        halo_copy(head).wait_send()
        u_s[slot, :HALO] = halo_in[lax.rem(head, EDGE_SLOTS)]

        @pl.when(head + 1 < n_heads)
        def _next_halo():
            halo_send(head + 1, tail_ref)

        for start in range(0, n_tok, BLOCK):
            u_s[slot, HALO + start:HALO + start + BLOCK] = jnp.swapaxes(u_ref[:, start:start + BLOCK, :].astype(jnp.float32), 0, 1)
            for tok in range(start, start + BLOCK):
                for lane in range(0, width, LANES):
                    cols = slice(lane, lane + LANES)
                    acc = par_ref[BC:BC + 1, cols] + par_ref[W0:W0 + 1, cols] * u_s[slot, tok + HALO, :, cols]
                    for tap in range(1, CONV):
                        acc = acc + par_ref[W0 + tap:W0 + tap + 1, cols] * (mask_ref[tap - 1, tok] * u_s[slot, tok + HALO - tap, :, cols])
                    c_s[slot, tok, :, cols] = acc
                    cb_s[slot, tok, :, cols] = acc.astype(jnp.bfloat16)
            g_s[slot, start:start + BLOCK] = jnp.swapaxes(gh_ref[:, start:start + BLOCK, :], 0, 1)
            part_c = cb_s[slot, start:start + BLOCK].reshape(rows, width)
            r_s[slot, start:start + BLOCK] = dot_nn(part_c, wa_ref[0]).reshape(BLOCK, n_batch, width)
            i_s[slot, start:start + BLOCK] = dot_nn(part_c, wi_ref[0]).reshape(BLOCK, n_batch, width)

        for half in range(width // LANES):
            cols = slice(half * LANES, (half + 1) * LANES)

            def fwd_body(chunk, run):
                state, prod = run
                base = chunk * STEPS
                for step in range(STEPS):
                    tok = base + step
                    gate_r = sigmoid_of(r_s[slot, tok, :, cols] + par_ref[BA:BA + 1, cols])
                    gate_i = sigmoid_of(i_s[slot, tok, :, cols] + par_ref[BI:BI + 1, cols])
                    decay, mult, ratio = decay_of(gate_r, par_ref[KE:KE + 1, cols], mask_ref[HALO, tok])
                    r_s[slot, tok, :, cols] = gate_r
                    i_s[slot, tok, :, cols] = gate_i
                    a_s[slot, tok, :, cols] = decay
                    m_s[slot, tok, :, cols] = mult
                    e_s[slot, tok, :, cols] = ratio
                    state = decay * state + mult * (gate_i * c_s[slot, tok, :, cols])
                    prod = decay * prod
                return state, prod

            zero = jnp.zeros((n_batch, LANES), jnp.float32)
            state, prod = lax.fori_loop(0, n_tok // STEPS, fwd_body, (zero, zero + 1.0))

            put_rows(head, 0, half, prod)
            put_rows(head, 1, half, state)

        def adj_body(chunk, adj):
            base = n_tok - STEPS - chunk * STEPS
            for step in reversed(range(STEPS)):
                tok = base + step
                adj = a_s[slot, tok] * (g_s[slot, tok] + adj)
            return adj

        first = lax.fori_loop(0, n_tok // STEPS, adj_body, jnp.zeros((n_batch, width), jnp.float32))
        for half in range(width // LANES):
            put_rows(head, 2, half, first[:, half * LANES:(half + 1) * LANES])
        spread(send, recv, send_sem, recv_sem, head, PITCH, SUM_ROWS)

    @pl.when((step_id >= 2) & (step_id <= n_heads + 1))
    def _combine():
        combine(step_id - 2)

    @pl.when((step_id >= 1) & (step_id <= n_heads))
    def _group():
        head = step_id - 1
        settle(recv, recv_sem, head, (GROUP - 1) * SUM_ROWS)
        prod = jnp.ones((4, LANES), jnp.float32)
        state = jnp.zeros((4, LANES), jnp.float32)
        adj = jnp.zeros((4, LANES), jnp.float32)
        for index in range(GROUP):
            decay = rows_of(recv, head, index, 0)
            state = decay * state + rows_of(recv, head, index, 1)
            prod = decay * prod
            other = GROUP - 1 - index
            adj = rows_of(recv, head, other, 0) * adj + rows_of(recv, head, other, 2)
        mine = block_of(z_at, PITCH, PITCH)
        group[head, mine, :] = jnp.concatenate([prod, state, adj, jnp.zeros_like(adj)], axis=0)
        for copy in group_copies(head):
            copy.start()

    for stage in reversed(range(1, STAGES + 1)):
        item_of = step_id - LAG - AFTER[stage]

        @pl.when((item_of >= 0) & (item_of < n_heads))
        def _sum(stage=stage, item_of=item_of):
            sum_stage(stage, item_of)

        @pl.when(item_of == n_heads - 1)
        def _sum_vectors(stage=stage):
            sum_stage(stage, n_heads)

    head_done = step_id - LAG - 3

    @pl.when((head_done >= 0) & (head_done < n_heads))
    def _stored():
        du_copy(head_done).wait()

    head_edge = step_id - LAG - 2

    @pl.when((head_edge >= 0) & (head_edge < n_heads))
    def _edge():
        slot = lax.rem(head_edge, EDGE_SLOTS)
        edge_copy(head_edge).wait_recv()
        edge_copy(head_edge).wait_send()
        du_s[slot, n_tok - HALO:] = (tail_s[slot] + edge_in[lax.rem(head_edge, EDGE_IN)]).astype(jnp.bfloat16)
        du_copy(head_edge).start()

    @pl.when((step_id >= LAG) & (step_id < n_heads + LAG))
    def _second():
        head = step_id - LAG
        slot = lax.rem(step_id - LAG, SLOTS)
        e_at = lax.rem(head, EDGE_SLOTS)
        settle(carry, take_sem, head, (GROUP - 1) * IN_ROWS)

        def state_body(chunk, state):
            base = chunk * STEPS
            for step in range(STEPS):
                tok = base + step
                h_scr[tok] = state
                state = a_s[slot, tok] * state + m_s[slot, tok] * (i_s[slot, tok] * c_s[slot, tok])
            return state

        state_in = [take_rows(head, 0, half) for half in range(width // LANES)]
        lax.fori_loop(0, n_tok // STEPS, state_body, jnp.concatenate(state_in, axis=1))

        for half in range(width // LANES):
            cols = slice(half * LANES, (half + 1) * LANES)
            zero8 = jnp.zeros((8, LANES), jnp.float32)

            def bwd_body(chunk, run):
                adj_next, sum_a, sum_i, sum_l = run
                base = n_tok - STEPS - chunk * STEPS
                for step in reversed(range(STEPS)):
                    tok = base + step
                    gate_r = r_s[slot, tok, :, cols]
                    gate_i = i_s[slot, tok, :, cols]
                    conv_c = c_s[slot, tok, :, cols]
                    adj = g_s[slot, tok, :, cols] + adj_next
                    adj_next = a_s[slot, tok, :, cols] * adj
                    direct = adj * m_s[slot, tok, :, cols] * gate_i
                    d_input = direct * conv_c
                    d_pre_i = d_input * (1.0 - gate_i)
                    d_log = adj_next * h_scr[tok, :, cols] - d_input * e_s[slot, tok, :, cols]
                    d_log_r = d_log * gate_r
                    d_pre_a = d_log_r * (par2_ref[KL:KL + 1, cols] * (1.0 - gate_r))
                    sum_l = sum_l + fold_rows(d_log_r)
                    sum_a = sum_a + fold_rows(d_pre_a)
                    sum_i = sum_i + fold_rows(d_pre_i)
                    d_scr[tok, :, cols] = direct
                    ga_scr[tok, :, cols] = d_pre_a.astype(jnp.bfloat16)
                    gi_scr[tok, :, cols] = d_pre_i.astype(jnp.bfloat16)
                return adj_next, sum_a, sum_i, sum_l

            adj_in = take_rows(head, 1, half)
            _, sum_a, sum_i, sum_l = lax.fori_loop(0, n_tok // STEPS, bwd_body, (adj_in, zero8, zero8, zero8))
            vec_ref[GBA:GBA + 1, cols] = jnp.sum(sum_a, axis=0, keepdims=True)
            vec_ref[GBI:GBI + 1, cols] = jnp.sum(sum_i, axis=0, keepdims=True)
            vec_ref[GLAM:GLAM + 1, cols] = jnp.sum(sum_l, axis=0, keepdims=True)

        p_at = lax.rem(head, PART_SLOTS)
        all_c = cb_s[slot].reshape(n_tok * n_batch, width)
        part[p_at, 0] = dot_tn(all_c, ga_scr[...].reshape(n_tok * n_batch, width))
        part[p_at, 1] = dot_tn(all_c, gi_scr[...].reshape(n_tok * n_batch, width))

        halves = width // LANES
        sums = [[jnp.zeros((8, LANES), jnp.float32)] * (CONV + 1) for _ in range(halves)]
        ahead = [[jnp.zeros((n_batch, LANES), jnp.float32)] * HALO for _ in range(halves)]
        for start in reversed(range(0, n_tok, BLOCK)):
            toks = slice(start, start + BLOCK)
            back = dot_nt(ga_scr[toks].reshape(rows, width), wa2_ref[0]) + dot_nt(gi_scr[toks].reshape(rows, width), wi2_ref[0])
            d_scr[toks] = d_scr[toks] + back.reshape(BLOCK, n_batch, width)
            for half in range(halves):
                cols = slice(half * LANES, (half + 1) * LANES)
                tot, nxt = sums[half], ahead[half]
                for tok in reversed(range(start, start + BLOCK)):
                    d_conv = d_scr[tok, :, cols]
                    tot[CONV] = tot[CONV] + fold_rows(d_conv)
                    masked = [d_conv] + [mask_ref[tap - 1, tok] * d_conv for tap in range(1, CONV)]
                    for tap in range(CONV):
                        tot[tap] = tot[tap] + fold_rows(masked[tap] * u_s[slot, tok + HALO - tap, :, cols])
                    terms = [par2_ref[W0 + tap:W0 + tap + 1, cols] * masked[tap] for tap in range(CONV)]
                    d_u = nxt[0] + terms[0]
                    du_s[e_at, tok, :, cols] = d_u.astype(jnp.bfloat16)
                    if tok >= n_tok - HALO:
                        tail_s[e_at, tok - n_tok + HALO, :, cols] = d_u
                    nxt = [nxt[1] + terms[1], nxt[2] + terms[2], terms[3]]
                ahead[half] = nxt
        for half in range(halves):
            cols = slice(half * LANES, (half + 1) * LANES)
            for row in range(CONV + 1):
                vec_ref[GW + row:GW + row + 1, cols] = jnp.sum(sums[half][row], axis=0, keepdims=True)
            for row in range(HALO):
                edge_out[e_at, HALO - 1 - row, :, cols] = ahead[half][row]
        edge_copy(head).start()
        vec_all[pl.ds(pl.multiple_of(head * N_VEC, N_VEC), N_VEC), :] = vec_ref[...]

    item_new = step_id - LAG

    @pl.when((item_new >= 0) & (item_new < n_heads))
    def _share():
        for copy in sum_copies(0, item_new):
            copy.start()

    @pl.when(item_new == n_heads - 1)
    def _share_vectors():
        p_at = n_heads % PART_SLOTS
        part[p_at, 0] = vec_all[...]
        part[p_at, 1] = jnp.zeros_like(vec_all)
        for copy in sum_copies(0, n_heads):
            copy.start()

    @pl.when(step_id == n_heads - 1 + LAG)
    def _drain():
        def one(head, _):
            settle(send, send_sem, head, (GROUP - 1) * SUM_ROWS)
            settle(resp, give_sem, head, (GROUP - 1) * IN_ROWS)
            return 0
        lax.fori_loop(0, n_heads, one, 0)


def solution(mesh):
    n_dev = mesh.shape['cp']
    seq_spec = P(None, 'cp', None)
    rep_spec = P()

    def local_fn(u_in, seg_ids, grad_h, conv_w, conv_b, a_gate_w, a_gate_b, x_gate_w, x_gate_b, lam_param):
        n_batch, n_tok, n_width = u_in.shape
        n_heads, block_w, _ = a_gate_w.shape
        seg_time = jnp.broadcast_to(seg_ids.T[:, :, None], (n_tok, n_batch, LANES))
        log_rate = -8.0 * jax.nn.softplus(-lam_param)
        par = jnp.concatenate([conv_w, conv_b[None], a_gate_b[None], x_gate_b[None], log_rate[None], log_rate[None] * LOG2E], axis=0)

        def now(step):
            return jnp.minimum(step, n_heads - 1)

        def late(step):
            return jnp.clip(step - LAG, 0, n_heads - 1)

        def blk_row(at):
            return pl.BlockSpec((n_batch, n_tok, block_w), lambda s: (0, 0, at(s)))

        tail_spec = pl.BlockSpec((n_batch, BLOCK, block_w), lambda s: (0, n_tok // BLOCK - 1, now(s + 1)))

        def mat_spec(at):
            return pl.BlockSpec((1, block_w, block_w), lambda s: (at(s), 0, 0))

        def par_spec(at):
            return pl.BlockSpec((N_PAR, block_w), lambda s: (0, at(s)))

        seg_spec = pl.BlockSpec((n_tok, n_batch, LANES), lambda s: (0, 0, 0), pipeline_mode=pl.Buffered(1))
        f32_slots = pltpu.VMEM((SLOTS, n_tok, n_batch, block_w), jnp.float32)
        f32_scr = pltpu.VMEM((n_tok, n_batch, block_w), jnp.float32)
        bf_scr = pltpu.VMEM((n_tok, n_batch, block_w), jnp.bfloat16)
        wire = pltpu.VMEM((n_heads, GROUP * PITCH, LANES), jnp.float32)
        half_wire = pltpu.VMEM((n_heads, GROUP * IN_ROWS, LANES), jnp.float32)
        sems = pltpu.SemaphoreType.DMA((n_heads,))

        item_f32 = functools.partial(pltpu.VMEM, dtype=jnp.float32)
        n_sems = 12
        du_time, grads = pl.pallas_call(
            functools.partial(fused_kernel, n_dev, n_heads), grid=(n_heads + LAG + AFTER[STAGES],),
            in_specs=[blk_row(now), tail_spec, blk_row(now), seg_spec, mat_spec(now), mat_spec(now),
                      mat_spec(late), mat_spec(late), par_spec(now), par_spec(late)],
            out_specs=[pl.BlockSpec(memory_space=pl.ANY)] * 2,
            out_shape=[jax.ShapeDtypeStruct((n_tok, n_batch, n_width), jnp.bfloat16),
                       jax.ShapeDtypeStruct((2, n_heads + 1, block_w, block_w), jnp.float32)],
            scratch_shapes=[pltpu.VMEM((SLOTS, n_tok + HALO, n_batch, block_w), jnp.float32)] + [f32_slots] * 7
            + [pltpu.VMEM((SLOTS, n_tok, n_batch, block_w), jnp.bfloat16), f32_scr, f32_scr, bf_scr, bf_scr] + [wire] * 2 + [half_wire] * 3
            + [item_f32((EDGE_SLOTS, HALO, n_batch, block_w))] * 2
            + [item_f32((HALO + 1, n_tok, n_batch, LANES)), pltpu.VMEM((HALO, n_batch, LANES), jnp.int32)]
            + [item_f32((PART_SLOTS, 2, block_w, block_w)), item_f32((FIRST_SLOTS, block_w, block_w)),
               item_f32((RECV_SLOTS, block_w // 2, block_w)), item_f32((RECV_SLOTS, block_w // 4, block_w)),
               item_f32((RECV_SLOTS, 3, block_w // 16, block_w)), item_f32((OWN_SLOTS, block_w, block_w)),
               item_f32((block_w, block_w)), item_f32((N_VEC, block_w)),
               pltpu.VMEM((EDGE_SLOTS, n_tok, n_batch, block_w), jnp.bfloat16)]
            + [item_f32((EDGE_SLOTS, HALO, n_batch, block_w))] * 2 + [item_f32((EDGE_IN, HALO, n_batch, block_w))]
            + [sems] * 2 + [pltpu.SemaphoreType.DMA((DEPTH - 1, n_heads))] * 2 + [sems] * 2 + [pltpu.SemaphoreType.DMA((EDGE_SLOTS,))] * 2
            + [pltpu.SemaphoreType.DMA((2,))]
            + [pltpu.SemaphoreType.DMA((n_sems, OWN_SLOTS))] * 2
            + [pltpu.SemaphoreType.DMA((count,)) for count in (EDGE_SLOTS, EDGE_IN, EDGE_SLOTS, OWN_SLOTS)],
            compiler_params=pltpu.CompilerParams(vmem_limit_bytes=67043328, has_side_effects=True), name='fused_pass',
        )(u_in, u_in, grad_h, seg_time, a_gate_w, x_gate_w, a_gate_w, x_gate_w, par, par)
        vecs = grads[0, n_heads, :n_heads * N_VEC].reshape(n_heads, N_VEC, block_w)
        vecs = jnp.swapaxes(vecs, 0, 1).reshape(N_VEC, n_width)
        g_lam = 8.0 * jax.nn.sigmoid(-lam_param) * vecs[GLAM]
        return (jnp.swapaxes(du_time, 0, 1), vecs[GW:GW + CONV], vecs[GBC], grads[0, :n_heads], vecs[GBA],
                grads[1, :n_heads], vecs[GBI], g_lam)

    return jax.shard_map(local_fn, mesh=mesh,
                         in_specs=(seq_spec, P(None, 'cp'), seq_spec, rep_spec, rep_spec, rep_spec,
                                   rep_spec, rep_spec, rep_spec, rep_spec),
                         out_specs=(seq_spec,) + (rep_spec,) * 7, check_vma=False)
```
